256 devices in a mesh: ctx: 32 (over y, z), chan: 8 (over x, core).
Axes of the slice: x: 4, y: 4, z: 8, core: 2. Of those that a mesh axis runs over, the one named last changes fastest.
Arguments:
- signal: bfloat16 [128, 262144], P('chan', 'ctx'), may hold values from -6 to 6
- filter_taps: bfloat16 [8, 262144], P('chan', 'ctx'), may hold values from -1 to 1
- gate_values: bfloat16 [128, 262144], P('chan', 'ctx'), may hold values from -6 to 6
- skip_weight: float32 [128], P('chan'), may hold values from -4 to 4
Outputs:
- gated_output: bfloat16 [128, 262144], P('chan', 'ctx')
The draws below stay inside these ranges and needn't reach their ends.
All inputs are finite; a program needn't handle non-finite values.
Results may differ from the reference program's by a relative error of at most 0.001.
Values may be sent and summed in bfloat16 or wider, within the bound.
A program may use at most 64 MiB of HBM per device.

```python
import math
import jax
import jax.numpy as jnp
from jax import lax

GROUP = 16
SEQ = 262144
CHANNELS = 128
FILTERS = 8


def draw_filter_taps(key, part):
    positions = jnp.arange(SEQ, dtype=jnp.float32)[None, :]

    def add_mode(mode_index, accum):
        subkeys = jax.random.split(jax.random.fold_in(key, mode_index), 5)
        slow_rate = jnp.exp(jax.random.uniform(subkeys[0], (FILTERS, 1), jnp.float32, math.log(0.5 / SEQ), math.log(2.0 / SEQ)))
        fast_rate = jnp.exp(jax.random.uniform(subkeys[1], (FILTERS, 1), jnp.float32, math.log(1.0 / 2000.0), math.log(1.0 / 30.0)))
        is_slow = jax.random.uniform(subkeys[4], (FILTERS, 1), jnp.float32) < 0.5
        decay_rate = jnp.where(is_slow, slow_rate, fast_rate)
        frequency = jax.random.uniform(subkeys[2], (FILTERS, 1), jnp.float32, 0.0, math.pi)
        offset_angle = jax.random.uniform(subkeys[3], (FILTERS, 1), jnp.float32, -math.pi, math.pi)
        amplitude = jax.random.normal(jax.random.fold_in(subkeys[3], 7), (FILTERS, 1), jnp.float32)
        return accum + amplitude * jnp.exp(-decay_rate * positions) * jnp.cos(frequency * positions + offset_angle)
    modal_sum = lax.fori_loop(0, 16, add_mode, jnp.zeros((FILTERS, SEQ), jnp.float32))
    rough_factor = jax.random.uniform(jax.random.fold_in(key, 1000), (FILTERS, SEQ), jnp.float32, 0.5, 1.5)
    tap_values = modal_sum * rough_factor
    row_norm = jnp.sqrt(jnp.sum(tap_values * tap_values, axis=1, keepdims=True))
    return (tap_values / row_norm).astype(jnp.bfloat16)


def levels(key, shape, shards, least, high):
    def one(dim, parts):
        heights = jax.random.uniform(jax.random.fold_in(jax.random.fold_in(key, 6), dim), (parts,), jnp.float32, least / len(shards), high / len(shards))
        return jnp.repeat(jnp.exp(heights), shape[dim] // parts).reshape((-1,) + (1,) * (len(shape) - dim - 1))

    factor_of = one(*shards[0])
    for cut in shards[1:]:
        factor_of = factor_of * one(*cut)
    return factor_of


def normal_values(own_key, shape, deviation, most, cuts=(), held_as=jnp.bfloat16):
    loudness = levels(own_key, shape, cuts, -0.22, 0.18) if cuts else 1.0
    values = jax.random.normal(own_key, shape, jnp.float32) * deviation * loudness
    return jnp.minimum(jnp.maximum(values, -most), most).astype(held_as)


def setup_inputs(seed: int = 0) -> dict:
    key_of = jax.random.split(jax.random.key(seed), 5)
    signal = normal_values(key_of[0], (CHANNELS, SEQ), 1.0, 6.0, ((0, 8), (1, 32)))
    filter_taps = draw_filter_taps(jax.random.fold_in(key_of[4], 71), 0)
    gate_values = normal_values(key_of[2], (CHANNELS, SEQ), 1.0, 6.0, ((0, 8), (1, 32)))
    skip_weight = normal_values(key_of[3], (CHANNELS,), 1.0, 4.0, ((0, 8),), jnp.float32)
    return dict(signal=signal, filter_taps=filter_taps, gate_values=gate_values, skip_weight=skip_weight)


def reference(signal, filter_taps, gate_values, skip_weight):
    seq_length = signal.shape[1]

    def convolve_row(channel):
        signal_row = signal[channel].astype(jnp.float32)
        tap_row = filter_taps[channel // GROUP].astype(jnp.float32)
        spectrum = jnp.fft.fft(jnp.pad(signal_row, (0, seq_length)))
        taps_spectrum = jnp.fft.fft(jnp.pad(tap_row, (0, seq_length)))
        return jnp.real(jnp.fft.ifft(spectrum * taps_spectrum))[:seq_length]

    convolved = lax.map(convolve_row, jnp.arange(CHANNELS, dtype=jnp.int32))
    mixed = gate_values.astype(jnp.float32) * (convolved + skip_weight[:, None] * signal.astype(jnp.float32))
    return mixed.astype(jnp.bfloat16)
```

```python
import functools

import jax
import jax.numpy as jnp
import ml_dtypes
import numpy as np
from jax import lax
from jax.experimental import pallas as pl
from jax.experimental.pallas import tpu as pltpu
from jax.sharding import Mesh
from jax.sharding import PartitionSpec as P

F32 = jnp.float32
BF16 = jnp.bfloat16
MESH = pl.DeviceIdType.MESH
PITCH = 136
HALF_ROOT = float(np.sqrt(0.5))


def two_parts(table):
    high = table.astype(ml_dtypes.bfloat16)
    low = (table - high.astype(np.float64)).astype(ml_dtypes.bfloat16)
    return np.stack([high, low])


@functools.cache
def tables():
    left, back, turn, step = [], [], [], []
    for core in range(2):
        shift = 0.125 + 0.5 * core
        kl = np.arange(128)[:, None] + shift
        angle = 2.0 * np.pi * np.mod(kl * np.arange(256)[None, :] / 128.0, 1.0)
        forward = np.concatenate([np.cos(angle), -np.sin(angle)], 0)
        left.append(two_parts(forward))
        inverse = np.roll(forward.T, -128 * core, 0)
        back.append(two_parts(inverse))
        angle = 2.0 * np.pi * np.mod(kl * np.arange(128)[None, :] / 131072.0, 1.0)
        turn.append(np.stack([np.cos(angle), -np.sin(angle)]))
        angle = np.broadcast_to(2.0 * np.pi * kl / 1024.0, (128, 128))
        step.append(np.stack([np.cos(angle), -np.sin(angle)]))
    index = np.arange(128)
    angle = 2.0 * np.pi * np.mod(index[:, None] * index[None, :] / 128.0, 1.0)
    cos, sin = np.cos(angle), np.sin(angle)
    right = two_parts(np.block([[cos, -sin], [sin, cos]]))
    undo = two_parts(np.block([[cos, sin], [-sin, cos]]) * 2.0**-18)
    angle = 2.0 * np.pi * np.arange(8)[:, None] * index[None, :] / 1024.0
    mid = np.stack([np.cos(angle), -np.sin(angle)])
    return (
        np.stack(left),
        np.stack(back),
        np.stack(turn).astype(np.float32),
        np.stack(step).astype(np.float32),
        right,
        undo,
        mid.astype(np.float32),
    )


def times(a, b):
    return (a[0] * b[0] - a[1] * b[1], a[0] * b[1] + a[1] * b[0])


def times_conj(a, b):
    return (a[0] * b[0] + a[1] * b[1], a[1] * b[0] - a[0] * b[1])


def plus(a, b):
    return (a[0] + b[0], a[1] + b[1])


def minus(a, b):
    return (a[0] - b[0], a[1] - b[1])


def quarter(a, sign):
    return (-a[1], a[0]) if sign > 0 else (a[1], -a[0])


def dft4(z, sign):
    even, odd = plus(z[0], z[2]), plus(z[1], z[3])
    d_even, d_odd = minus(z[0], z[2]), quarter(minus(z[1], z[3]), sign)
    return [plus(even, odd), plus(d_even, d_odd), minus(even, odd), minus(d_even, d_odd)]


def dft8(z, sign):
    low = [plus(z[j], z[j + 4]) for j in range(4)]
    high = [minus(z[j], z[j + 4]) for j in range(4)]
    h1 = plus(high[1], quarter(high[1], sign))
    h3 = minus(quarter(high[3], sign), high[3])
    high = [
        high[0],
        (h1[0] * HALF_ROOT, h1[1] * HALF_ROOT),
        quarter(high[2], sign),
        (h3[0] * HALF_ROOT, h3[1] * HALF_ROOT),
    ]
    even, odd = dft4(low, sign), dft4(high, sign)
    return [even[0], odd[0], even[1], odd[1], even[2], odd[2], even[3], odd[3]]


def split(value):
    high = value.astype(BF16)
    return high, (value - high.astype(F32)).astype(BF16)


def mm(a, b):
    return jnp.dot(a, b, preferred_element_type=F32)


def make_turns(turn, step, turns):
    def body(q, carry):
        rows = pl.ds(pl.multiple_of(q * 16, 16), 16)
        now = (turn[0, rows, :], turn[1, rows, :])
        by = (step[0, rows, :], step[1, rows, :])
        for a in range(8):
            turns[0, a, rows, :] = now[0]
            turns[1, a, rows, :] = now[1]
            if a < 7:
                now = times(now, by)
        return carry

    lax.fori_loop(0, 8, body, 0)


def forward_front(data, left, turns, mid, grid_f32, c_high, c_low):
    for c in range(4):
        tile = data[:, 16 * c : 16 * c + 16, :].astype(F32)
        block = jnp.concatenate(
            [tile[:, :8, :].reshape(256, 128), tile[:, 8:, :].reshape(256, 128)], axis=1
        ).astype(BF16)
        grid_f32[:, 256 * c : 256 * c + 256] = mm(left[0], block) + mm(left[1], block)

    def body(q, carry):
        at = pl.multiple_of(q * 16, 16)
        z = []
        for a in range(8):
            cols = slice(128 * a, 128 * a + 128)
            value = (grid_f32[pl.ds(at, 16), cols], grid_f32[pl.ds(at + 128, 16), cols])
            z.append(times(value, (turns[0, a, pl.ds(at, 16), :], turns[1, a, pl.ds(at, 16), :])))
        z = dft8(z, -1)
        for ka in range(8):
            value = z[ka]
            if ka:
                value = times(value, (mid[0, ka : ka + 1, :], mid[1, ka : ka + 1, :]))
            rows = pl.ds(pl.multiple_of(at + 128 * ka, 16), 16)
            for part in range(2):
                cols = slice(128 * part, 128 * part + 128)
                c_high[rows, cols], c_low[rows, cols] = split(value[part])
        return carry

    lax.fori_loop(0, 8, body, 0)


def taps_spectrum(right, c_high, c_low, spectrum):
    for m in range(4):
        rows = slice(256 * m, 256 * m + 256)
        high, low = c_high[rows, :], c_low[rows, :]
        spectrum[rows, :] = mm(high, right[0]) + mm(low, right[0]) + mm(high, right[1])


def middle(right, undo, c_high, c_low, spectrum, back_grid):
    for m in range(4):
        rows = slice(256 * m, 256 * m + 256)
        high, low = c_high[rows, :], c_low[rows, :]
        value = mm(high, right[0]) + mm(low, right[0]) + mm(high, right[1])
        taps = spectrum[rows, :]
        re, im = times((value[:, :128], value[:, 128:]), (taps[:, :128], taps[:, 128:]))
        high, low = split(jnp.concatenate([re, im], axis=1))
        back_grid[rows, :] = mm(high, undo[0]) + mm(low, undo[0]) + mm(high, undo[1])


def inverse_back(turns, mid, back_grid, d_high, d_low):
    def body(q, carry):
        at = pl.multiple_of(q * 16, 16)
        z = []
        for ka in range(8):
            rows = pl.ds(pl.multiple_of(at + 128 * ka, 16), 16)
            value = (back_grid[rows, 0:128], back_grid[rows, 128:256])
            if ka:
                value = times_conj(value, (mid[0, ka : ka + 1, :], mid[1, ka : ka + 1, :]))
            z.append(value)
        z = dft8(z, 1)
        for a in range(8):
            value = times_conj(z[a], (turns[0, a, pl.ds(at, 16), :], turns[1, a, pl.ds(at, 16), :]))
            cols = slice(128 * a, 128 * a + 128)
            for part in range(2):
                rows = pl.ds(pl.multiple_of(at + 128 * part, 16), 16)
                d_high[rows, cols], d_low[rows, cols] = split(value[part])
        return carry

    lax.fori_loop(0, 8, body, 0)


def inverse_columns(c, back, d_high, d_low):
    cols = slice(256 * c, 256 * c + 256)
    high, low = d_high[:, cols], d_low[:, cols]
    return mm(back[0], high) + mm(back[0], low) + mm(back[1], high)


def spread_out(rows_ref, work, send):
    for j in range(64):
        at = (j // 8) * PITCH + (j % 8) * 16
        work[at : at + 16, :] = rows_ref[:, 128 * j : 128 * j + 128].astype(F32)
    for r in range(16):
        for a in range(0, 8, 2):
            pair = [work[pl.ds((a + o) * 16 + r, 8, stride=PITCH), :] for o in range(2)]
            send[r, 8 * a : 8 * a + 16, :] = jnp.concatenate(pair, axis=0).astype(BF16)


def put_back(received, work, out_ref):
    for r in range(16):
        for a in range(0, 8, 2):
            pair = received[r, 8 * a : 8 * a + 16, :].astype(F32)
            for o in range(2):
                work[pl.ds((a + o) * 16 + r, 8, stride=PITCH), :] = pair[8 * o : 8 * o + 8, :]
    for j in range(64):
        at = (j // 8) * PITCH + (j % 8) * 16
        out_ref[:, 128 * j : 128 * j + 128] = work[at : at + 16, :].astype(BF16)


def kernel(
    signal, taps, gate, skip, left_all, back_all, turn_all, step_all, right_all, undo_all, mid_all, out,
    left, back, turn, step, right, undo, mid,
    work, taps_work, send_x, send_g, send_t, recv_x, recv_t, recv_g, send_o, recv_o, skips,
    turns, grid_f32, c_high, c_low, spectrum, back_grid, d_high, d_low, y_mine, y_send, y_recv,
    table_sems, sx, rx, st, rt, sg, rg, so, ro, fsx, frx, fst, frt, sy, ry, skip_sems,
):
    shard = lax.axis_index("ctx")
    core = lax.axis_index("core")
    half = lax.div(shard, 16)
    spot = lax.rem(shard, 16)
    first = 16 * core
    other = 16 - first
    mate = {"core": 1 - core}

    copies = []
    for i, (src, dst) in enumerate(
        [
            (left_all.at[core], left),
            (back_all.at[core], back),
            (turn_all.at[core], turn),
            (step_all.at[core], step),
            (right_all, right),
            (undo_all, undo),
            (mid_all, mid),
        ]
    ):
        copies.append(pltpu.make_async_copy(src, dst, table_sems.at[i]))
        copies[-1].start()

    barrier = pltpu.get_barrier_semaphore()

    def greet(i, carry):
        @pl.when(first + i != shard)
        def _():
            pl.semaphore_signal(
                barrier, inc=1, device_id={"ctx": first + i, "core": half}, device_id_type=MESH
            )

        return carry

    lax.fori_loop(0, 16, greet, 0)
    pl.semaphore_signal(barrier, inc=1, device_id=mate, device_id_type=MESH)

    for j in range(64):
        row = (j % 8) * 8 + j // 8
        taps_work[row : row + 1, :] = taps[:, 128 * j : 128 * j + 128].astype(F32)
    send_t[...] = taps_work[...].astype(BF16)
    spread_out(signal, work, send_x)
    spread_out(gate, work, send_g)
    for r in range(16):
        skips[core, r : r + 1, :] = jnp.full((1, 128), skip[r], F32)

    pl.semaphore_wait(barrier, jnp.where(core == half, 16, 17))

    def peer_copy(i, src, dst, send_sem, recv_sem):
        return pltpu.make_async_remote_copy(
            src_ref=src,
            dst_ref=dst,
            send_sem=send_sem.at[i],
            recv_sem=recv_sem,
            device_id={"ctx": first + i, "core": half},
            device_id_type=MESH,
        )

    def each_peer(remote, here=None):
        def body(k, carry):
            i = lax.rem(spot + k, 16)

            @pl.when(first + i != shard)
            def _():
                remote(i)

            if here is not None:

                @pl.when(first + i == shard)
                def _():
                    here(i)

            return carry

        lax.fori_loop(0, 16, body, 0)

    def out_t(i):
        return peer_copy(i, send_t, recv_t.at[shard], st, rt.at[spot])

    def out_x(i):
        return peer_copy(i, send_x.at[i], recv_x.at[shard], sx, rx.at[spot])

    def out_g(i):
        return peer_copy(i, send_g.at[i], recv_g.at[spot], sg, rg.at[spot])

    def out_o(i):
        return peer_copy(i, send_o.at[i], recv_o.at[spot], so, ro.at[spot])

    def keep_t(i):
        recv_t[shard] = send_t[...]

    def keep_x(i):
        recv_x[shard] = send_x[i]

    def keep_g(i):
        recv_g[spot] = send_g[i]

    skip_copy = pltpu.make_async_remote_copy(
        src_ref=skips.at[core], dst_ref=skips.at[core], send_sem=skip_sems.at[0],
        recv_sem=skip_sems.at[1], device_id=mate, device_id_type=MESH,
    )
    each_peer(lambda i: out_t(i).start(), keep_t)
    each_peer(lambda i: out_x(i).start(), keep_x)
    each_peer(lambda i: out_g(i).start(), keep_g)
    skip_copy.start()

    def incoming(i, src, slot, recv_sem):
        return pltpu.make_async_remote_copy(
            src_ref=src, dst_ref=slot, send_sem=st.at[i], recv_sem=recv_sem.at[i],
            device_id={"ctx": first + i, "core": half}, device_id_type=MESH,
        )

    def to_mate(i, ref, slot, send_sem, recv_sem):
        return pltpu.make_async_remote_copy(
            src_ref=ref.at[slot], dst_ref=ref.at[slot], send_sem=send_sem.at[i],
            recv_sem=recv_sem.at[i], device_id=mate, device_id_type=MESH,
        )

    def gather(ref, recv_sem, fwd_send, fwd_recv):
        def pass_on(k, carry):
            i = lax.rem(spot + k, 16)

            @pl.when(first + i != shard)
            def _():
                incoming(i, send_t, ref.at[first + i], recv_sem).wait_recv()

            to_mate(i, ref, first + i, fwd_send, fwd_recv).start()
            return carry

        lax.fori_loop(0, 16, pass_on, 0)

        def take(i, carry):
            to_mate(i, ref, other + i, fwd_send, fwd_recv).wait_recv()
            return carry

        lax.fori_loop(0, 16, take, 0)

    for copy in copies:
        copy.wait()
    make_turns(turn, step, turns)

    gather(recv_t, rt, fst, frt)
    forward_front(recv_t, left, turns, mid, grid_f32, c_high, c_low)
    taps_spectrum(right, c_high, c_low, spectrum)
    gather(recv_x, rx, fsx, frx)
    forward_front(recv_x, left, turns, mid, grid_f32, c_high, c_low)
    middle(right, undo, c_high, c_low, spectrum, back_grid)
    inverse_back(turns, mid, back_grid, d_high, d_low)

    def y_copy(c):
        return pltpu.make_async_remote_copy(
            src_ref=y_send.at[c], dst_ref=y_recv.at[c], send_sem=sy.at[c], recv_sem=ry.at[c],
            device_id=mate, device_id_type=MESH,
        )

    for c in range(4):
        value = inverse_columns(c, back, d_high, d_low)
        y_send[c] = value[128:, :]
        y_mine[c] = value[:128, :]
        y_copy(c).start()
    skip_copy.wait()
    weight = skips[half, pl.ds(spot, 1), :]
    each_peer(lambda i: incoming(i, send_t, recv_g.at[i], rg).wait_recv())
    for c in range(4):
        y_copy(c).wait_recv()

    def finish(i):
        rows = pl.ds(pl.multiple_of(i * 8, 8), 8)
        for c in range(4):
            total = y_mine[c, rows, :] + y_recv[c, rows, :]
            total = jnp.concatenate([total[:, :128], total[:, 128:]], axis=0)
            cut = slice(16 * c, 16 * c + 16)
            direct = recv_x[first + i, cut, :].astype(F32)
            total = recv_g[i, cut, :].astype(F32) * (total + weight * direct)
            send_o[i, cut, :] = total.astype(BF16)

    def send_back(i):
        finish(i)
        out_o(i).start()

    def keep_o(i):
        finish(i)
        recv_o[spot] = send_o[i]

    each_peer(send_back, keep_o)
    each_peer(lambda i: incoming(i, send_t, recv_o.at[i], ro).wait_recv())
    put_back(recv_o, work, out)

    def sent(i):
        out_t(i).wait_send()
        out_x(i).wait_send()
        out_g(i).wait_send()
        out_o(i).wait_send()

    each_peer(sent)

    def passed(i, carry):
        to_mate(i, recv_t, first + i, fst, frt).wait_send()
        to_mate(i, recv_x, first + i, fsx, frx).wait_send()
        return carry

    lax.fori_loop(0, 16, passed, 0)
    for c in range(4):
        y_copy(c).wait_send()


def local(signal, filter_taps, gate_values, skip_weight):
    held = tables()
    vmem, dma = pltpu.VMEM, pltpu.SemaphoreType.DMA
    whole = pl.BlockSpec(memory_space=pltpu.VMEM)
    apart = pl.BlockSpec(memory_space=pl.ANY)
    scratch = [
        vmem((2, 256, 256), BF16),
        vmem((2, 256, 256), BF16),
        vmem((2, 128, 128), F32),
        vmem((2, 128, 128), F32),
        vmem((2, 256, 256), BF16),
        vmem((2, 256, 256), BF16),
        vmem((2, 8, 128), F32),
        vmem((8 * PITCH, 128), F32),
        vmem((64, 128), F32),
        vmem((16, 64, 128), BF16),
        vmem((16, 64, 128), BF16),
        vmem((64, 128), BF16),
        vmem((32, 64, 128), BF16),
        vmem((32, 64, 128), BF16),
        vmem((16, 64, 128), BF16),
        vmem((16, 64, 128), BF16),
        vmem((16, 64, 128), BF16),
        vmem((2, 16, 128), F32),
        vmem((2, 8, 128, 128), F32),
        vmem((256, 1024), F32),
        vmem((1024, 256), BF16),
        vmem((1024, 256), BF16),
        vmem((1024, 256), F32),
        vmem((1024, 256), F32),
        vmem((256, 1024), BF16),
        vmem((256, 1024), BF16),
        vmem((4, 128, 256), F32),
        vmem((4, 128, 256), F32),
        vmem((4, 128, 256), F32),
        dma((7,)),
        *[dma((16,)) for _ in range(12)],
        dma((4,)),
        dma((4,)),
        dma((2,)),
    ]
    return pl.pallas_call(
        kernel,
        out_shape=jax.ShapeDtypeStruct(signal.shape, BF16),
        in_specs=[whole, whole, whole, pl.BlockSpec(memory_space=pltpu.SMEM)] + [apart] * len(held),
        out_specs=whole,
        scratch_shapes=scratch,
        compiler_params=pltpu.CompilerParams(collective_id=0, has_side_effects=True),
        name="hyena",
    )(signal, filter_taps, gate_values, skip_weight, *[jnp.asarray(t) for t in held])


def solution(mesh):
    shards = mesh.shape["ctx"]
    finer = Mesh(mesh.devices.reshape(shards, -1, 2), ("ctx", "x", "core"))
    chan = ("x", "core")
    placed = (P(chan, "ctx"), P(chan, "ctx"), P(chan, "ctx"), P(chan))
    return jax.shard_map(
        local, mesh=finer, in_specs=placed, out_specs=P(chan, "ctx"), check_vma=False
    )
```

```python
import functools

import jax
import jax.numpy as jnp
import ml_dtypes
import numpy as np
from jax import lax
from jax.experimental import pallas as pl
from jax.experimental.pallas import tpu as pltpu
from jax.sharding import Mesh
from jax.sharding import PartitionSpec as P

F32 = jnp.float32
BF16 = jnp.bfloat16
MESH = pl.DeviceIdType.MESH
PITCH = 136
HALF_ROOT = float(np.sqrt(0.5))


def two_parts(table):
    high = table.astype(ml_dtypes.bfloat16)
    low = (table - high.astype(np.float64)).astype(ml_dtypes.bfloat16)
    return np.stack([high, low])


@functools.cache
def tables():
    left, back, turn, step = [], [], [], []
    for core in range(2):
        shift = 0.125 + 0.5 * core
        kl = np.arange(128)[:, None] + shift
        angle = 2.0 * np.pi * np.mod(kl * np.arange(256)[None, :] / 128.0, 1.0)
        forward = np.concatenate([np.cos(angle), -np.sin(angle)], 0)
        left.append(two_parts(forward))
        inverse = np.roll(forward.T, -128 * core, 0)
        back.append(two_parts(inverse))
        angle = 2.0 * np.pi * np.mod(kl * np.arange(128)[None, :] / 131072.0, 1.0)
        turn.append(np.stack([np.cos(angle), -np.sin(angle)]))
        angle = np.broadcast_to(2.0 * np.pi * kl / 1024.0, (128, 128))
        step.append(np.stack([np.cos(angle), -np.sin(angle)]))
    index = np.arange(128)
    angle = 2.0 * np.pi * np.mod(index[:, None] * index[None, :] / 128.0, 1.0)
    cos, sin = np.cos(angle), np.sin(angle)
    right = two_parts(np.block([[cos, -sin], [sin, cos]]))
    undo = two_parts(np.block([[cos, sin], [-sin, cos]]) * 2.0**-18)
    angle = 2.0 * np.pi * np.arange(8)[:, None] * index[None, :] / 1024.0
    mid = np.stack([np.cos(angle), -np.sin(angle)])
    return (
        np.stack(left),
        np.stack(back),
        np.stack(turn).astype(np.float32),
        np.stack(step).astype(np.float32),
        right,
        undo,
        mid.astype(np.float32),
    )


def times(a, b):
    return (a[0] * b[0] - a[1] * b[1], a[0] * b[1] + a[1] * b[0])


def times_conj(a, b):
    return (a[0] * b[0] + a[1] * b[1], a[1] * b[0] - a[0] * b[1])


def plus(a, b):
    return (a[0] + b[0], a[1] + b[1])


def minus(a, b):
    return (a[0] - b[0], a[1] - b[1])


def quarter(a, sign):
    return (-a[1], a[0]) if sign > 0 else (a[1], -a[0])


def dft4(z, sign):
    even, odd = plus(z[0], z[2]), plus(z[1], z[3])
    d_even, d_odd = minus(z[0], z[2]), quarter(minus(z[1], z[3]), sign)
    return [plus(even, odd), plus(d_even, d_odd), minus(even, odd), minus(d_even, d_odd)]


def dft8(z, sign):
    low = [plus(z[j], z[j + 4]) for j in range(4)]
    high = [minus(z[j], z[j + 4]) for j in range(4)]
    h1 = plus(high[1], quarter(high[1], sign))
    h3 = minus(quarter(high[3], sign), high[3])
    high = [
        high[0],
        (h1[0] * HALF_ROOT, h1[1] * HALF_ROOT),
        quarter(high[2], sign),
        (h3[0] * HALF_ROOT, h3[1] * HALF_ROOT),
    ]
    even, odd = dft4(low, sign), dft4(high, sign)
    return [even[0], odd[0], even[1], odd[1], even[2], odd[2], even[3], odd[3]]


def split(value):
    high = value.astype(BF16)
    return high, (value - high.astype(F32)).astype(BF16)


def mm(a, b):
    return jnp.dot(a, b, preferred_element_type=F32)


def make_turns(turn, step, turns):
    def body(q, carry):
        rows = pl.ds(pl.multiple_of(q * 16, 16), 16)
        now = (turn[0, rows, :], turn[1, rows, :])
        by = (step[0, rows, :], step[1, rows, :])
        for a in range(8):
            turns[0, a, rows, :] = now[0]
            turns[1, a, rows, :] = now[1]
            if a < 7:
                now = times(now, by)
        return carry

    lax.fori_loop(0, 8, body, 0)


def forward_front(data, left, turns, mid, grid_f32, c_high, c_low):
    for c in range(4):
        tile = data[:, 16 * c : 16 * c + 16, :].astype(F32)
        block = jnp.concatenate(
            [tile[:, :8, :].reshape(256, 128), tile[:, 8:, :].reshape(256, 128)], axis=1
        ).astype(BF16)
        grid_f32[:, 256 * c : 256 * c + 256] = mm(left[0], block) + mm(left[1], block)

    def body(q, carry):
        at = pl.multiple_of(q * 16, 16)
        z = []
        for a in range(8):
            cols = slice(128 * a, 128 * a + 128)
            value = (grid_f32[pl.ds(at, 16), cols], grid_f32[pl.ds(at + 128, 16), cols])
            z.append(times(value, (turns[0, a, pl.ds(at, 16), :], turns[1, a, pl.ds(at, 16), :])))
        z = dft8(z, -1)
        for ka in range(8):
            value = z[ka]
            if ka:
                value = times(value, (mid[0, ka : ka + 1, :], mid[1, ka : ka + 1, :]))
            rows = pl.ds(pl.multiple_of(at + 128 * ka, 16), 16)
            for part in range(2):
                cols = slice(128 * part, 128 * part + 128)
                c_high[rows, cols], c_low[rows, cols] = split(value[part])
        return carry

    lax.fori_loop(0, 8, body, 0)


def taps_spectrum(right, c_high, c_low, spectrum):
    for m in range(4):
        rows = slice(256 * m, 256 * m + 256)
        high, low = c_high[rows, :], c_low[rows, :]
        spectrum[rows, :] = mm(high, right[0]) + mm(low, right[0]) + mm(high, right[1])


def middle(right, undo, c_high, c_low, spectrum, back_grid):
    for m in range(4):
        rows = slice(256 * m, 256 * m + 256)
        high, low = c_high[rows, :], c_low[rows, :]
        value = mm(high, right[0]) + mm(low, right[0]) + mm(high, right[1])
        taps = spectrum[rows, :]
        re, im = times((value[:, :128], value[:, 128:]), (taps[:, :128], taps[:, 128:]))
        high, low = split(jnp.concatenate([re, im], axis=1))
        back_grid[rows, :] = mm(high, undo[0]) + mm(low, undo[0]) + mm(high, undo[1])


def inverse_back(turns, mid, back_grid, d_high, d_low):
    def body(q, carry):
        at = pl.multiple_of(q * 16, 16)
        z = []
        for ka in range(8):
            rows = pl.ds(pl.multiple_of(at + 128 * ka, 16), 16)
            value = (back_grid[rows, 0:128], back_grid[rows, 128:256])
            if ka:
                value = times_conj(value, (mid[0, ka : ka + 1, :], mid[1, ka : ka + 1, :]))
            z.append(value)
        z = dft8(z, 1)
        for a in range(8):
            value = times_conj(z[a], (turns[0, a, pl.ds(at, 16), :], turns[1, a, pl.ds(at, 16), :]))
            cols = slice(128 * a, 128 * a + 128)
            for part in range(2):
                rows = pl.ds(pl.multiple_of(at + 128 * part, 16), 16)
                d_high[rows, cols], d_low[rows, cols] = split(value[part])
        return carry

    lax.fori_loop(0, 8, body, 0)


def inverse_columns(c, back, d_high, d_low):
    cols = slice(256 * c, 256 * c + 256)
    high, low = d_high[:, cols], d_low[:, cols]
    return mm(back[0], high) + mm(back[0], low) + mm(back[1], high)


def spread_out(rows_ref, work, send):
    for j in range(64):
        at = (j // 8) * PITCH + (j % 8) * 16
        work[at : at + 16, :] = rows_ref[:, 128 * j : 128 * j + 128].astype(F32)
    for r in range(16):
        for a in range(0, 8, 2):
            pair = [work[pl.ds((a + o) * 16 + r, 8, stride=PITCH), :] for o in range(2)]
            send[r, 8 * a : 8 * a + 16, :] = jnp.concatenate(pair, axis=0).astype(BF16)


def put_row(received, work, r):
    for a in range(0, 8, 2):
        pair = received[r, 8 * a : 8 * a + 16, :].astype(F32)
        for o in range(2):
            work[pl.ds((a + o) * 16 + r, 8, stride=PITCH), :] = pair[8 * o : 8 * o + 8, :]


def start_order(ctx, core):
    z, y = lax.rem(ctx, 8), lax.div(ctx, 8)
    return (jnp.minimum(z, 4) * 10 + y * 6 + (1 - core) * 4) * 64 + ctx * 2 + core


def kernel(
    signal_in, taps_in, gate_in, skip_in, left_all, back_all, turn_all, step_all, right_all, undo_all, mid_all,
    out_all,
    signal, taps, gate, skip, out,
    left, back, turn, step, right, undo, mid,
    work, taps_work, send_x, send_g, send_t, recv_x, recv_t, recv_g, send_o, recv_o, skips,
    turns, grid_f32, c_high, c_low, spectrum, back_grid, d_high, d_low, y_mine, y_send, y_recv,
    input_sems, table_sems, out_sems,
    sx, rx, st, rt, sg, rg, so, ro, fsx, frx, fst, frt, sy, ry, skip_sems, ready,
):
    shard = lax.axis_index("ctx")
    core = lax.axis_index("core")
    half = lax.div(shard, 16)
    spot = lax.rem(shard, 16)
    first = 16 * core
    other = 16 - first
    mate = {"core": 1 - core}
    mine = start_order(shard, core)
    mate_later = start_order(shard, 1 - core) > mine

    def peer_later(i):
        return start_order(first + i, half) > mine

    def peer_earlier(i):
        return start_order(first + i, half) < mine

    def peer(i):
        return {"ctx": first + i, "core": half}

    def all_peers(body):
        def run(k, carry):
            body(lax.rem(spot + k, 16))
            return carry

        lax.fori_loop(0, 16, run, 0)

    barrier = pltpu.get_barrier_semaphore()

    def greet(i):
        @pl.when(peer_later(i))
        def _():
            pl.semaphore_signal(barrier, inc=1, device_id=peer(i), device_id_type=MESH)

    all_peers(greet)

    @pl.when(mate_later)
    def _():
        pl.semaphore_signal(barrier, inc=1, device_id=mate, device_id_type=MESH)

    def fetch(pairs, sems):
        copies = [pltpu.make_async_copy(a, b, sems.at[i]) for i, (a, b) in enumerate(pairs)]
        for copy in copies:
            copy.start()
        return copies

    inputs = fetch(
        [(taps_in, taps), (signal_in, signal), (gate_in, gate), (skip_in, skip)], input_sems
    )
    copies = fetch(
        [
            (left_all.at[core], left),
            (turn_all.at[core], turn),
            (step_all.at[core], step),
            (right_all, right),
            (mid_all, mid),
            (undo_all, undo),
            (back_all.at[core], back),
        ],
        table_sems,
    )

    inputs[0].wait()
    for j in range(64):
        row = (j % 8) * 8 + j // 8
        taps_work[row : row + 1, :] = taps[:, 128 * j : 128 * j + 128].astype(F32)
    send_t[...] = taps_work[...].astype(BF16)
    inputs[1].wait()
    spread_out(signal, work, send_x)

    earlier = lax.fori_loop(
        0, 16, lambda i, n: n + jnp.where(peer_earlier(i), 1, 0), jnp.where(mate_later, 0, 1)
    )

    @pl.when(earlier > 0)
    def _():
        pl.semaphore_wait(barrier, earlier)

    def answer(i):
        @pl.when(peer_earlier(i))
        def _():
            pl.semaphore_signal(ready.at[spot], inc=1, device_id=peer(i), device_id_type=MESH)

    all_peers(answer)

    @pl.when(jnp.logical_not(mate_later))
    def _():
        pl.semaphore_signal(ready.at[16], inc=1, device_id=mate, device_id_type=MESH)

    def peer_copy(i, src, dst, send_sem, recv_sem):
        return pltpu.make_async_remote_copy(
            src_ref=src, dst_ref=dst, send_sem=send_sem.at[i], recv_sem=recv_sem,
            device_id=peer(i), device_id_type=MESH,
        )

    def others(body):
        def run(i):
            @pl.when(first + i != shard)
            def _():
                body(i)

        all_peers(run)

    def out_t(i):
        return peer_copy(i, send_t, recv_t.at[shard], st, rt.at[spot])

    def out_x(i):
        return peer_copy(i, send_x.at[i], recv_x.at[shard], sx, rx.at[spot])

    def out_g(i):
        return peer_copy(i, send_g.at[i], recv_g.at[spot], sg, rg.at[spot])

    def out_o(i):
        return peer_copy(i, send_o.at[i], recv_o.at[spot], so, ro.at[spot])

    def if_earlier(body):
        def run(i):
            @pl.when(peer_earlier(i))
            def _():
                body(i)

        return run

    all_peers(if_earlier(lambda i: out_t(i).start()))
    all_peers(if_earlier(lambda i: out_x(i).start()))

    @pl.when(core == half)
    def _():
        recv_t[shard] = send_t[...]
        recv_x[shard] = send_x[spot]

    def later_in_turn(k, carry):
        i = lax.rem(k, 2) * 8 + lax.div(k, 2)

        @pl.when(peer_later(i))
        def _():
            pl.semaphore_wait(ready.at[i], 1)
            out_t(i).start()
            out_x(i).start()

        return carry

    lax.fori_loop(0, 16, later_in_turn, 0)

    @pl.when(mate_later)
    def _():
        pl.semaphore_wait(ready.at[16], 1)

    inputs[2].wait()
    spread_out(gate, work, send_g)
    others(lambda i: out_g(i).start())

    @pl.when(core == half)
    def _():
        recv_g[spot] = send_g[spot]

    inputs[3].wait()
    for r in range(16):
        skips[core, r : r + 1, :] = jnp.full((1, 128), skip[r], F32)
    skip_copy = pltpu.make_async_remote_copy(
        src_ref=skips.at[core], dst_ref=skips.at[core], send_sem=skip_sems.at[0],
        recv_sem=skip_sems.at[1], device_id=mate, device_id_type=MESH,
    )
    skip_copy.start()

    def incoming(i, slot, recv_sem):
        return peer_copy(i, send_t, slot, st, recv_sem.at[i])

    def to_mate(i, ref, slot, send_sem, recv_sem):
        return pltpu.make_async_remote_copy(
            src_ref=ref.at[slot], dst_ref=ref.at[slot], send_sem=send_sem.at[i],
            recv_sem=recv_sem.at[i], device_id=mate, device_id_type=MESH,
        )

    def gather(ref, recv_sem, fwd_send, fwd_recv):
        def pass_on(i):
            @pl.when(first + i != shard)
            def _():
                incoming(i, ref.at[first + i], recv_sem).wait_recv()

            to_mate(i, ref, first + i, fwd_send, fwd_recv).start()

        all_peers(pass_on)

        def take(i, carry):
            to_mate(i, ref, other + i, fwd_send, fwd_recv).wait_recv()
            return carry

        lax.fori_loop(0, 16, take, 0)

    for copy in copies:
        copy.wait()
    make_turns(turn, step, turns)

    gather(recv_t, rt, fst, frt)
    forward_front(recv_t, left, turns, mid, grid_f32, c_high, c_low)
    taps_spectrum(right, c_high, c_low, spectrum)
    gather(recv_x, rx, fsx, frx)
    forward_front(recv_x, left, turns, mid, grid_f32, c_high, c_low)
    middle(right, undo, c_high, c_low, spectrum, back_grid)
    inverse_back(turns, mid, back_grid, d_high, d_low)

    def y_copy(c):
        return pltpu.make_async_remote_copy(
            src_ref=y_send.at[c], dst_ref=y_recv.at[c], send_sem=sy.at[c], recv_sem=ry.at[c],
            device_id=mate, device_id_type=MESH,
        )

    for c in range(4):
        value = inverse_columns(c, back, d_high, d_low)
        y_send[c] = value[128:, :]
        y_mine[c] = value[:128, :]
        y_copy(c).start()
    skip_copy.wait()
    weight = skips[half, pl.ds(spot, 1), :]
    others(lambda i: incoming(i, recv_g.at[i], rg).wait_recv())
    for c in range(4):
        y_copy(c).wait_recv()

    def send_back(i):
        rows = pl.ds(pl.multiple_of(i * 8, 8), 8)
        for c in range(4):
            total = y_mine[c, rows, :] + y_recv[c, rows, :]
            total = jnp.concatenate([total[:, :128], total[:, 128:]], axis=0)
            cut = slice(16 * c, 16 * c + 16)
            direct = recv_x[first + i, cut, :].astype(F32)
            total = recv_g[i, cut, :].astype(F32) * (total + weight * direct)
            send_o[i, cut, :] = total.astype(BF16)

        @pl.when(first + i != shard)
        def _():
            out_o(i).start()

        @pl.when(first + i == shard)
        def _():
            recv_o[spot] = send_o[i]

    all_peers(send_back)

    def place(i):
        @pl.when(first + i != shard)
        def _():
            incoming(i, recv_o.at[i], ro).wait_recv()

        put_row(recv_o, work, i)

    all_peers(place)
    results = []
    for piece in range(4):
        for j in range(16 * piece, 16 * piece + 16):
            at = (j // 8) * PITCH + (j % 8) * 16
            out[piece, :, 128 * (j % 16) : 128 * (j % 16) + 128] = work[at : at + 16, :].astype(BF16)
        cols = slice(2048 * piece, 2048 * piece + 2048)
        results.append(pltpu.make_async_copy(out.at[piece], out_all.at[:, cols], out_sems.at[piece]))
        results[-1].start()

    def sent(i):
        out_t(i).wait_send()
        out_x(i).wait_send()
        out_g(i).wait_send()
        out_o(i).wait_send()

    others(sent)

    def passed(i, carry):
        to_mate(i, recv_t, first + i, fst, frt).wait_send()
        to_mate(i, recv_x, first + i, fsx, frx).wait_send()
        return carry

    lax.fori_loop(0, 16, passed, 0)
    for c in range(4):
        y_copy(c).wait_send()
    for result in results:
        result.wait()


def local(signal, filter_taps, gate_values, skip_weight):
    held = tables()
    vmem, dma = pltpu.VMEM, pltpu.SemaphoreType.DMA
    apart = pl.BlockSpec(memory_space=pl.ANY)
    scratch = [
        vmem((16, 8192), BF16),
        vmem((1, 8192), BF16),
        vmem((16, 8192), BF16),
        pltpu.SMEM((16,), F32),
        vmem((4, 16, 2048), BF16),
        vmem((2, 256, 256), BF16),
        vmem((2, 256, 256), BF16),
        vmem((2, 128, 128), F32),
        vmem((2, 128, 128), F32),
        vmem((2, 256, 256), BF16),
        vmem((2, 256, 256), BF16),
        vmem((2, 8, 128), F32),
        vmem((8 * PITCH, 128), F32),
        vmem((64, 128), F32),
        vmem((16, 64, 128), BF16),
        vmem((16, 64, 128), BF16),
        vmem((64, 128), BF16),
        vmem((32, 64, 128), BF16),
        vmem((32, 64, 128), BF16),
        vmem((16, 64, 128), BF16),
        vmem((16, 64, 128), BF16),
        vmem((16, 64, 128), BF16),
        vmem((2, 16, 128), F32),
        vmem((2, 8, 128, 128), F32),
        vmem((256, 1024), F32),
        vmem((1024, 256), BF16),
        vmem((1024, 256), BF16),
        vmem((1024, 256), F32),
        vmem((1024, 256), F32),
        vmem((256, 1024), BF16),
        vmem((256, 1024), BF16),
        vmem((4, 128, 256), F32),
        vmem((4, 128, 256), F32),
        vmem((4, 128, 256), F32),
        dma((4,)),
        dma((7,)),
        dma((4,)),
        *[dma((16,)) for _ in range(12)],
        dma((4,)),
        dma((4,)),
        dma((2,)),
        pltpu.SemaphoreType.REGULAR((17,)),
    ]
    return pl.pallas_call(
        kernel,
        out_shape=jax.ShapeDtypeStruct(signal.shape, BF16),
        in_specs=[apart] * (4 + len(held)),
        out_specs=apart,
        scratch_shapes=scratch,
        compiler_params=pltpu.CompilerParams(collective_id=0, has_side_effects=True),
        name="hyena",
    )(signal, filter_taps, gate_values, skip_weight, *[jnp.asarray(t) for t in held])


def solution(mesh):
    shards = mesh.shape["ctx"]
    finer = Mesh(mesh.devices.reshape(shards, -1, 2), ("ctx", "x", "core"))
    chan = ("x", "core")
    placed = (P(chan, "ctx"), P(chan, "ctx"), P(chan, "ctx"), P(chan))
    return jax.shard_map(
        local, mesh=finer, in_specs=placed, out_specs=P(chan, "ctx"), check_vma=False
    )
```

```python
import functools

import jax
import jax.numpy as jnp
import ml_dtypes
import numpy as np
from jax import lax
from jax.experimental import pallas as pl
from jax.experimental.pallas import tpu as pltpu
from jax.sharding import Mesh
from jax.sharding import PartitionSpec as P

F32 = jnp.float32
BF16 = jnp.bfloat16
MESH = pl.DeviceIdType.MESH
PITCH = 136
HALF_ROOT = float(np.sqrt(0.5))


def two_parts(table):
    high = table.astype(ml_dtypes.bfloat16)
    low = (table - high.astype(np.float64)).astype(ml_dtypes.bfloat16)
    return np.stack([high, low])


@functools.cache
def tables():
    left, back, turn, step = [], [], [], []
    for core in range(2):
        shift = 0.125 + 0.5 * core
        kl = np.arange(128)[:, None] + shift
        angle = 2.0 * np.pi * np.mod(kl * np.arange(256)[None, :] / 128.0, 1.0)
        forward = np.concatenate([np.cos(angle), -np.sin(angle)], 0)
        left.append(two_parts(forward))
        inverse = np.roll(forward.T, -128 * core, 0)
        back.append(two_parts(inverse))
        angle = 2.0 * np.pi * np.mod(kl * np.arange(128)[None, :] / 131072.0, 1.0)
        turn.append(np.stack([np.cos(angle), -np.sin(angle)]))
        angle = np.broadcast_to(2.0 * np.pi * kl / 1024.0, (128, 128))
        step.append(np.stack([np.cos(angle), -np.sin(angle)]))
    index = np.arange(128)
    angle = 2.0 * np.pi * np.mod(index[:, None] * index[None, :] / 128.0, 1.0)
    cos, sin = np.cos(angle), np.sin(angle)
    right = two_parts(np.block([[cos, -sin], [sin, cos]]))
    undo = two_parts(np.block([[cos, sin], [-sin, cos]]) * 2.0**-18)
    angle = 2.0 * np.pi * np.arange(8)[:, None] * index[None, :] / 1024.0
    mid = np.stack([np.cos(angle), -np.sin(angle)])
    return (
        np.stack(left),
        np.stack(back),
        np.stack(turn).astype(np.float32),
        np.stack(step).astype(np.float32),
        right,
        undo,
        mid.astype(np.float32),
    )


def times(a, b):
    return (a[0] * b[0] - a[1] * b[1], a[0] * b[1] + a[1] * b[0])


def times_conj(a, b):
    return (a[0] * b[0] + a[1] * b[1], a[1] * b[0] - a[0] * b[1])


def plus(a, b):
    return (a[0] + b[0], a[1] + b[1])


def minus(a, b):
    return (a[0] - b[0], a[1] - b[1])


def quarter(a, sign):
    return (-a[1], a[0]) if sign > 0 else (a[1], -a[0])


def dft4(z, sign):
    even, odd = plus(z[0], z[2]), plus(z[1], z[3])
    d_even, d_odd = minus(z[0], z[2]), quarter(minus(z[1], z[3]), sign)
    return [plus(even, odd), plus(d_even, d_odd), minus(even, odd), minus(d_even, d_odd)]


def dft8(z, sign):
    low = [plus(z[j], z[j + 4]) for j in range(4)]
    high = [minus(z[j], z[j + 4]) for j in range(4)]
    h1 = plus(high[1], quarter(high[1], sign))
    h3 = minus(quarter(high[3], sign), high[3])
    high = [
        high[0],
        (h1[0] * HALF_ROOT, h1[1] * HALF_ROOT),
        quarter(high[2], sign),
        (h3[0] * HALF_ROOT, h3[1] * HALF_ROOT),
    ]
    even, odd = dft4(low, sign), dft4(high, sign)
    return [even[0], odd[0], even[1], odd[1], even[2], odd[2], even[3], odd[3]]


def split(value):
    high = value.astype(BF16)
    return high, (value - high.astype(F32)).astype(BF16)


def mm(a, b):
    return jnp.dot(a, b, preferred_element_type=F32)


def make_turns(turn, step, turns):
    def body(q, carry):
        rows = pl.ds(pl.multiple_of(q * 16, 16), 16)
        now = (turn[0, rows, :], turn[1, rows, :])
        by = (step[0, rows, :], step[1, rows, :])
        for a in range(8):
            turns[0, a, rows, :] = now[0]
            turns[1, a, rows, :] = now[1]
            if a < 7:
                now = times(now, by)
        return carry

    lax.fori_loop(0, 8, body, 0)


def forward_front(data, left, turns, mid, grid_f32, c_high, c_low):
    for c in range(4):
        tile = data[:, 16 * c : 16 * c + 16, :].astype(F32)
        block = jnp.concatenate(
            [tile[:, :8, :].reshape(256, 128), tile[:, 8:, :].reshape(256, 128)], axis=1
        ).astype(BF16)
        grid_f32[:, 256 * c : 256 * c + 256] = mm(left[0], block) + mm(left[1], block)

    def body(q, carry):
        at = pl.multiple_of(q * 16, 16)
        z = []
        for a in range(8):
            cols = slice(128 * a, 128 * a + 128)
            value = (grid_f32[pl.ds(at, 16), cols], grid_f32[pl.ds(at + 128, 16), cols])
            z.append(times(value, (turns[0, a, pl.ds(at, 16), :], turns[1, a, pl.ds(at, 16), :])))
        z = dft8(z, -1)
        for ka in range(8):
            value = z[ka]
            if ka:
                value = times(value, (mid[0, ka : ka + 1, :], mid[1, ka : ka + 1, :]))
            rows = pl.ds(pl.multiple_of(at + 128 * ka, 16), 16)
            for part in range(2):
                cols = slice(128 * part, 128 * part + 128)
                c_high[rows, cols], c_low[rows, cols] = split(value[part])
        return carry

    lax.fori_loop(0, 8, body, 0)


def taps_spectrum(right, c_high, c_low, spectrum):
    for m in range(4):
        rows = slice(256 * m, 256 * m + 256)
        high, low = c_high[rows, :], c_low[rows, :]
        spectrum[rows, :] = mm(high, right[0]) + mm(low, right[0]) + mm(high, right[1])


def middle(right, undo, c_high, c_low, spectrum, back_grid):
    for m in range(4):
        rows = slice(256 * m, 256 * m + 256)
        high, low = c_high[rows, :], c_low[rows, :]
        value = mm(high, right[0]) + mm(low, right[0]) + mm(high, right[1])
        taps = spectrum[rows, :]
        re, im = times((value[:, :128], value[:, 128:]), (taps[:, :128], taps[:, 128:]))
        high, low = split(jnp.concatenate([re, im], axis=1))
        back_grid[rows, :] = mm(high, undo[0]) + mm(low, undo[0]) + mm(high, undo[1])


def inverse_back(turns, mid, back_grid, d_high, d_low):
    def body(q, carry):
        at = pl.multiple_of(q * 16, 16)
        z = []
        for ka in range(8):
            rows = pl.ds(pl.multiple_of(at + 128 * ka, 16), 16)
            value = (back_grid[rows, 0:128], back_grid[rows, 128:256])
            if ka:
                value = times_conj(value, (mid[0, ka : ka + 1, :], mid[1, ka : ka + 1, :]))
            z.append(value)
        z = dft8(z, 1)
        for a in range(8):
            value = times_conj(z[a], (turns[0, a, pl.ds(at, 16), :], turns[1, a, pl.ds(at, 16), :]))
            cols = slice(128 * a, 128 * a + 128)
            for part in range(2):
                rows = pl.ds(pl.multiple_of(at + 128 * part, 16), 16)
                d_high[rows, cols], d_low[rows, cols] = split(value[part])
        return carry

    lax.fori_loop(0, 8, body, 0)


def inverse_columns(c, back, d_high, d_low):
    cols = slice(256 * c, 256 * c + 256)
    high, low = d_high[:, cols], d_low[:, cols]
    return mm(back[0], high) + mm(back[0], low) + mm(back[1], high)


def spread_out(rows_ref, work, send):
    for j in range(64):
        at = (j // 8) * PITCH + (j % 8) * 16
        work[at : at + 16, :] = rows_ref[:, 128 * j : 128 * j + 128].astype(F32)
    for r in range(16):
        for a in range(0, 8, 2):
            pair = [work[pl.ds((a + o) * 16 + r, 8, stride=PITCH), :] for o in range(2)]
            send[r, 8 * a : 8 * a + 16, :] = jnp.concatenate(pair, axis=0).astype(BF16)


def put_row(received, work, r):
    for a in range(0, 8, 2):
        pair = received[r, 8 * a : 8 * a + 16, :].astype(F32)
        for o in range(2):
            work[pl.ds((a + o) * 16 + r, 8, stride=PITCH), :] = pair[8 * o : 8 * o + 8, :]


def kernel(
    signal_in, taps_in, gate_in, skip_in, left_all, back_all, turn_all, step_all, right_all, undo_all, mid_all,
    out_all,
    signal, taps, gate, skip, out,
    left, back, turn, step, right, undo, mid,
    work, taps_work, send_x, send_g, send_t, ring_t, recv_x, recv_t, recv_g, send_o, recv_o, skips,
    turns, grid_f32, c_high, c_low, spectrum, back_grid, d_high, d_low, y_mine, y_send, y_recv,
    input_sems, table_sems, out_sems,
    sr, rr, sx, rx, st, rt, sg, rg, so, ro, fsx, frx, fst, frt, sy, ry, skip_sems,
):
    shard = lax.axis_index("ctx")
    core = lax.axis_index("core")
    half = lax.div(shard, 16)
    spot = lax.rem(shard, 16)
    first = 16 * core
    other = 16 - first
    mate = {"core": 1 - core}
    row = lax.div(shard, 8)
    col = lax.rem(shard, 8)

    def peer(i):
        return {"ctx": first + i, "core": half}

    def all_peers(body):
        def run(k, carry):
            body(lax.rem(spot + k, 16))
            return carry

        lax.fori_loop(0, 16, run, 0)

    barrier = pltpu.get_barrier_semaphore()

    def others(body):
        def run(i):
            @pl.when(first + i != shard)
            def _():
                body(i)

        all_peers(run)

    def ring(i):
        return {"ctx": row * 8 + i}

    def along_ring(body):
        def run(k, carry):
            body(lax.rem(col + k, 8))
            return carry

        lax.fori_loop(1, 8, run, 0)

    def hello(device):
        pl.semaphore_signal(barrier, inc=1, device_id=device, device_id_type=MESH)

    others(lambda i: hello(peer(i)))
    hello(mate)

    @pl.when(core != half)
    def _():
        along_ring(lambda i: hello(ring(i)))

    def fetch(pairs, sems):
        copies = [pltpu.make_async_copy(a, b, sems.at[i]) for i, (a, b) in enumerate(pairs)]
        for copy in copies:
            copy.start()
        return copies

    inputs = fetch(
        [(taps_in, taps), (signal_in, signal), (gate_in, gate), (skip_in, skip)], input_sems
    )
    copies = fetch(
        [
            (left_all.at[core], left),
            (turn_all.at[core], turn),
            (step_all.at[core], step),
            (right_all, right),
            (mid_all, mid),
            (undo_all, undo),
            (back_all.at[core], back),
        ],
        table_sems,
    )

    inputs[0].wait()
    for j in range(64):
        at = (j % 8) * 8 + j // 8
        taps_work[at : at + 1, :] = taps[:, 128 * j : 128 * j + 128].astype(F32)
    send_t[...] = taps_work[...].astype(BF16)
    inputs[1].wait()
    spread_out(signal, work, send_x)

    pl.semaphore_wait(barrier, jnp.where(core == half, 16, 24))

    def peer_copy(i, src, dst, send_sem, recv_sem):
        return pltpu.make_async_remote_copy(
            src_ref=src, dst_ref=dst, send_sem=send_sem.at[i], recv_sem=recv_sem,
            device_id=peer(i), device_id_type=MESH,
        )

    def ring_copy(i, slot):
        return pltpu.make_async_remote_copy(
            src_ref=send_t, dst_ref=ring_t.at[slot], send_sem=sr.at[i], recv_sem=rr.at[slot],
            device_id=ring(i), device_id_type=MESH,
        )

    def row_copy(block, side):
        i = side * 8 + col
        return pltpu.make_async_remote_copy(
            src_ref=ring_t.at[block], dst_ref=recv_t.at[row * 8 + block], send_sem=st.at[side * 8 + block],
            recv_sem=rt.at[lax.rem(row, 2) * 8 + block], device_id=peer(i), device_id_type=MESH,
        )

    def out_x(i):
        return peer_copy(i, send_x.at[i], recv_x.at[shard], sx, rx.at[spot])

    def out_g(i):
        return peer_copy(i, send_g.at[i], recv_g.at[spot], sg, rg.at[spot])

    def out_o(i):
        return peer_copy(i, send_o.at[i], recv_o.at[spot], so, ro.at[spot])

    along_ring(lambda i: ring_copy(i, col).start())
    ring_t[col] = send_t[...]
    others(lambda i: out_x(i).start())

    @pl.when(core == half)
    def _():
        recv_x[shard] = send_x[spot]

    inputs[2].wait()
    spread_out(gate, work, send_g)
    others(lambda i: out_g(i).start())

    @pl.when(core == half)
    def _():
        recv_g[spot] = send_g[spot]

    inputs[3].wait()
    for r in range(16):
        skips[core, r : r + 1, :] = jnp.full((1, 128), skip[r], F32)
    skip_copy = pltpu.make_async_remote_copy(
        src_ref=skips.at[core], dst_ref=skips.at[core], send_sem=skip_sems.at[0],
        recv_sem=skip_sems.at[1], device_id=mate, device_id_type=MESH,
    )
    skip_copy.start()

    def incoming(i, slot, recv_sem):
        return peer_copy(i, send_t, slot, sx, recv_sem.at[i])

    def to_rows(block):
        for side in range(2):

            @pl.when(first + side * 8 + col != shard)
            def _():
                row_copy(block, side).start()

        @pl.when(core == half)
        def _():
            recv_t[row * 8 + block] = ring_t[block]

    to_rows(col)

    def relay(i):
        ring_copy(i, i).wait_recv()
        to_rows(i)

    along_ring(relay)

    def to_mate(i, ref, slot, send_sem, recv_sem):
        return pltpu.make_async_remote_copy(
            src_ref=ref.at[slot], dst_ref=ref.at[slot], send_sem=send_sem.at[i],
            recv_sem=recv_sem.at[i], device_id=mate, device_id_type=MESH,
        )

    def gather(ref, recv_sem, fwd_send, fwd_recv, remote):
        def pass_on(i):
            @pl.when(remote(i))
            def _():
                incoming(i, ref.at[first + i], recv_sem).wait_recv()

            to_mate(i, ref, first + i, fwd_send, fwd_recv).start()

        all_peers(pass_on)

        def take(i, carry):
            to_mate(i, ref, other + i, fwd_send, fwd_recv).wait_recv()
            return carry

        lax.fori_loop(0, 16, take, 0)

    for copy in copies:
        copy.wait()
    make_turns(turn, step, turns)

    gather(recv_t, rt, fst, frt, lambda i: lax.div(first + i, 8) != row)
    forward_front(recv_t, left, turns, mid, grid_f32, c_high, c_low)
    taps_spectrum(right, c_high, c_low, spectrum)
    gather(recv_x, rx, fsx, frx, lambda i: first + i != shard)
    forward_front(recv_x, left, turns, mid, grid_f32, c_high, c_low)
    middle(right, undo, c_high, c_low, spectrum, back_grid)
    inverse_back(turns, mid, back_grid, d_high, d_low)

    def y_copy(c):
        return pltpu.make_async_remote_copy(
            src_ref=y_send.at[c], dst_ref=y_recv.at[c], send_sem=sy.at[c], recv_sem=ry.at[c],
            device_id=mate, device_id_type=MESH,
        )

    for c in range(4):
        value = inverse_columns(c, back, d_high, d_low)
        y_send[c] = value[128:, :]
        y_mine[c] = value[:128, :]
        y_copy(c).start()
    skip_copy.wait()
    weight = skips[half, pl.ds(spot, 1), :]
    others(lambda i: incoming(i, recv_g.at[i], rg).wait_recv())
    for c in range(4):
        y_copy(c).wait_recv()

    def send_back(i):
        rows = pl.ds(pl.multiple_of(i * 8, 8), 8)
        for c in range(4):
            total = y_mine[c, rows, :] + y_recv[c, rows, :]
            total = jnp.concatenate([total[:, :128], total[:, 128:]], axis=0)
            cut = slice(16 * c, 16 * c + 16)
            direct = recv_x[first + i, cut, :].astype(F32)
            total = recv_g[i, cut, :].astype(F32) * (total + weight * direct)
            send_o[i, cut, :] = total.astype(BF16)

        @pl.when(first + i != shard)
        def _():
            out_o(i).start()

        @pl.when(first + i == shard)
        def _():
            recv_o[spot] = send_o[i]

    all_peers(send_back)

    def place(i):
        @pl.when(first + i != shard)
        def _():
            incoming(i, recv_o.at[i], ro).wait_recv()

        put_row(recv_o, work, i)

    all_peers(place)
    results = []
    for piece in range(4):
        for j in range(16 * piece, 16 * piece + 16):
            at = (j // 8) * PITCH + (j % 8) * 16
            out[piece, :, 128 * (j % 16) : 128 * (j % 16) + 128] = work[at : at + 16, :].astype(BF16)
        cols = slice(2048 * piece, 2048 * piece + 2048)
        results.append(pltpu.make_async_copy(out.at[piece], out_all.at[:, cols], out_sems.at[piece]))
        results[-1].start()

    def sent(i):
        out_x(i).wait_send()
        out_g(i).wait_send()
        out_o(i).wait_send()

    others(sent)
    along_ring(lambda i: ring_copy(i, col).wait_send())

    def rows_sent(block, carry):
        for side in range(2):

            @pl.when(first + side * 8 + col != shard)
            def _():
                row_copy(block, side).wait_send()

        return carry

    lax.fori_loop(0, 8, rows_sent, 0)

    def passed(i, carry):
        to_mate(i, recv_t, first + i, fst, frt).wait_send()
        to_mate(i, recv_x, first + i, fsx, frx).wait_send()
        return carry

    lax.fori_loop(0, 16, passed, 0)
    for c in range(4):
        y_copy(c).wait_send()
    for result in results:
        result.wait()


def local(signal, filter_taps, gate_values, skip_weight):
    held = tables()
    vmem, dma = pltpu.VMEM, pltpu.SemaphoreType.DMA
    apart = pl.BlockSpec(memory_space=pl.ANY)
    scratch = [
        vmem((16, 8192), BF16),
        vmem((1, 8192), BF16),
        vmem((16, 8192), BF16),
        pltpu.SMEM((16,), F32),
        vmem((4, 16, 2048), BF16),
        vmem((2, 256, 256), BF16),
        vmem((2, 256, 256), BF16),
        vmem((2, 128, 128), F32),
        vmem((2, 128, 128), F32),
        vmem((2, 256, 256), BF16),
        vmem((2, 256, 256), BF16),
        vmem((2, 8, 128), F32),
        vmem((8 * PITCH, 128), F32),
        vmem((64, 128), F32),
        vmem((16, 64, 128), BF16),
        vmem((16, 64, 128), BF16),
        vmem((64, 128), BF16),
        vmem((8, 64, 128), BF16),
        vmem((32, 64, 128), BF16),
        vmem((32, 64, 128), BF16),
        vmem((16, 64, 128), BF16),
        vmem((16, 64, 128), BF16),
        vmem((16, 64, 128), BF16),
        vmem((2, 16, 128), F32),
        vmem((2, 8, 128, 128), F32),
        vmem((256, 1024), F32),
        vmem((1024, 256), BF16),
        vmem((1024, 256), BF16),
        vmem((1024, 256), F32),
        vmem((1024, 256), F32),
        vmem((256, 1024), BF16),
        vmem((256, 1024), BF16),
        vmem((4, 128, 256), F32),
        vmem((4, 128, 256), F32),
        vmem((4, 128, 256), F32),
        dma((4,)),
        dma((7,)),
        dma((4,)),
        dma((8,)),
        dma((8,)),
        *[dma((16,)) for _ in range(12)],
        dma((4,)),
        dma((4,)),
        dma((2,)),
    ]
    return pl.pallas_call(
        kernel,
        out_shape=jax.ShapeDtypeStruct(signal.shape, BF16),
        in_specs=[apart] * (4 + len(held)),
        out_specs=apart,
        scratch_shapes=scratch,
        compiler_params=pltpu.CompilerParams(collective_id=0, has_side_effects=True),
        name="hyena",
    )(signal, filter_taps, gate_values, skip_weight, *[jnp.asarray(t) for t in held])


def solution(mesh):
    shards = mesh.shape["ctx"]
    finer = Mesh(mesh.devices.reshape(shards, -1, 2), ("ctx", "x", "core"))
    chan = ("x", "core")
    placed = (P(chan, "ctx"), P(chan, "ctx"), P(chan, "ctx"), P(chan))
    return jax.shard_map(
        local, mesh=finer, in_specs=placed, out_specs=P(chan, "ctx"), check_vma=False
    )
```

```python
import functools

import jax
import jax.numpy as jnp
import ml_dtypes
import numpy as np
from jax import lax
from jax.experimental import pallas as pl
from jax.experimental.pallas import tpu as pltpu
from jax.sharding import Mesh
from jax.sharding import PartitionSpec as P

F32 = jnp.float32
BF16 = jnp.bfloat16
MESH = pl.DeviceIdType.MESH
PITCH = 136
HALF_ROOT = float(np.sqrt(0.5))


def two_parts(table):
    high = table.astype(ml_dtypes.bfloat16)
    low = (table - high.astype(np.float64)).astype(ml_dtypes.bfloat16)
    return np.stack([high, low])


@functools.cache
def tables():
    left, back, turn, step = [], [], [], []
    for core in range(2):
        shift = 0.125 + 0.5 * core
        kl = np.arange(128)[:, None] + shift
        angle = 2.0 * np.pi * np.mod(kl * np.arange(256)[None, :] / 128.0, 1.0)
        forward = np.concatenate([np.cos(angle), -np.sin(angle)], 0)
        left.append(two_parts(forward))
        inverse = np.roll(forward.T, -128 * core, 0)
        back.append(two_parts(inverse))
        angle = 2.0 * np.pi * np.mod(kl * np.arange(128)[None, :] / 131072.0, 1.0)
        turn.append(np.stack([np.cos(angle), -np.sin(angle)]))
        angle = np.broadcast_to(2.0 * np.pi * kl / 1024.0, (128, 128))
        step.append(np.stack([np.cos(angle), -np.sin(angle)]))
    index = np.arange(128)
    angle = 2.0 * np.pi * np.mod(index[:, None] * index[None, :] / 128.0, 1.0)
    cos, sin = np.cos(angle), np.sin(angle)
    right = two_parts(np.block([[cos, -sin], [sin, cos]]))
    undo = two_parts(np.block([[cos, sin], [-sin, cos]]) * 2.0**-18)
    angle = 2.0 * np.pi * np.arange(8)[:, None] * index[None, :] / 1024.0
    mid = np.stack([np.cos(angle), -np.sin(angle)])
    return (
        np.stack(left),
        np.stack(back),
        np.stack(turn).astype(np.float32),
        np.stack(step).astype(np.float32),
        right,
        undo,
        mid.astype(np.float32),
    )


def times(a, b):
    return (a[0] * b[0] - a[1] * b[1], a[0] * b[1] + a[1] * b[0])


def times_conj(a, b):
    return (a[0] * b[0] + a[1] * b[1], a[1] * b[0] - a[0] * b[1])


def plus(a, b):
    return (a[0] + b[0], a[1] + b[1])


def minus(a, b):
    return (a[0] - b[0], a[1] - b[1])


def quarter(a, sign):
    return (-a[1], a[0]) if sign > 0 else (a[1], -a[0])


def dft4(z, sign):
    even, odd = plus(z[0], z[2]), plus(z[1], z[3])
    d_even, d_odd = minus(z[0], z[2]), quarter(minus(z[1], z[3]), sign)
    return [plus(even, odd), plus(d_even, d_odd), minus(even, odd), minus(d_even, d_odd)]


def dft8(z, sign):
    low = [plus(z[j], z[j + 4]) for j in range(4)]
    high = [minus(z[j], z[j + 4]) for j in range(4)]
    h1 = plus(high[1], quarter(high[1], sign))
    h3 = minus(quarter(high[3], sign), high[3])
    high = [
        high[0],
        (h1[0] * HALF_ROOT, h1[1] * HALF_ROOT),
        quarter(high[2], sign),
        (h3[0] * HALF_ROOT, h3[1] * HALF_ROOT),
    ]
    even, odd = dft4(low, sign), dft4(high, sign)
    return [even[0], odd[0], even[1], odd[1], even[2], odd[2], even[3], odd[3]]


def split(value):
    high = value.astype(BF16)
    return high, (value - high.astype(F32)).astype(BF16)


def mm(a, b):
    return jnp.dot(a, b, preferred_element_type=F32)


def make_turns(turn, step, turns):
    def body(q, carry):
        rows = pl.ds(pl.multiple_of(q * 16, 16), 16)
        now = (turn[0, rows, :], turn[1, rows, :])
        by = (step[0, rows, :], step[1, rows, :])
        for a in range(8):
            turns[0, a, rows, :] = now[0]
            turns[1, a, rows, :] = now[1]
            if a < 7:
                now = times(now, by)
        return carry

    lax.fori_loop(0, 8, body, 0)


def forward_front(data, left, turns, mid, grid_f32, c_high, c_low):
    for c in range(4):
        tile = data[:, 16 * c : 16 * c + 16, :].astype(F32)
        block = jnp.concatenate(
            [tile[:, :8, :].reshape(256, 128), tile[:, 8:, :].reshape(256, 128)], axis=1
        ).astype(BF16)
        grid_f32[:, 256 * c : 256 * c + 256] = mm(left[0], block) + mm(left[1], block)

    def body(q, carry):
        at = pl.multiple_of(q * 16, 16)
        z = []
        for a in range(8):
            cols = slice(128 * a, 128 * a + 128)
            value = (grid_f32[pl.ds(at, 16), cols], grid_f32[pl.ds(at + 128, 16), cols])
            z.append(times(value, (turns[0, a, pl.ds(at, 16), :], turns[1, a, pl.ds(at, 16), :])))
        z = dft8(z, -1)
        for ka in range(8):
            value = z[ka]
            if ka:
                value = times(value, (mid[0, ka : ka + 1, :], mid[1, ka : ka + 1, :]))
            rows = pl.ds(pl.multiple_of(at + 128 * ka, 16), 16)
            for part in range(2):
                cols = slice(128 * part, 128 * part + 128)
                c_high[rows, cols], c_low[rows, cols] = split(value[part])
        return carry

    lax.fori_loop(0, 8, body, 0)


def spectrum_of(right, c_high, c_low, spectrum):
    for m in range(4):
        rows = slice(256 * m, 256 * m + 256)
        high, low = c_high[rows, :], c_low[rows, :]
        spectrum[rows, :] = mm(high, right[0]) + mm(low, right[0]) + mm(high, right[1])


def middle(right, undo, c_high, c_low, spectrum, back_grid):
    for m in range(4):
        rows = slice(256 * m, 256 * m + 256)
        high, low = c_high[rows, :], c_low[rows, :]
        value = mm(high, right[0]) + mm(low, right[0]) + mm(high, right[1])
        taps = spectrum[rows, :]
        re, im = times((value[:, :128], value[:, 128:]), (taps[:, :128], taps[:, 128:]))
        high, low = split(jnp.concatenate([re, im], axis=1))
        back_grid[rows, :] = mm(high, undo[0]) + mm(low, undo[0]) + mm(high, undo[1])


def inverse_back(turns, mid, back_grid, d_high, d_low):
    def body(q, carry):
        at = pl.multiple_of(q * 16, 16)
        z = []
        for ka in range(8):
            rows = pl.ds(pl.multiple_of(at + 128 * ka, 16), 16)
            value = (back_grid[rows, 0:128], back_grid[rows, 128:256])
            if ka:
                value = times_conj(value, (mid[0, ka : ka + 1, :], mid[1, ka : ka + 1, :]))
            z.append(value)
        z = dft8(z, 1)
        for a in range(8):
            value = times_conj(z[a], (turns[0, a, pl.ds(at, 16), :], turns[1, a, pl.ds(at, 16), :]))
            cols = slice(128 * a, 128 * a + 128)
            for part in range(2):
                rows = pl.ds(pl.multiple_of(at + 128 * part, 16), 16)
                d_high[rows, cols], d_low[rows, cols] = split(value[part])
        return carry

    lax.fori_loop(0, 8, body, 0)


def inverse_columns(c, back, d_high, d_low):
    cols = slice(256 * c, 256 * c + 256)
    high, low = d_high[:, cols], d_low[:, cols]
    return mm(back[0], high) + mm(back[0], low) + mm(back[1], high)


def spread_out(rows_ref, work, send):
    for j in range(64):
        at = (j // 8) * PITCH + (j % 8) * 16
        work[at : at + 16, :] = rows_ref[:, 128 * j : 128 * j + 128].astype(F32)
    for r in range(16):
        for a in range(0, 8, 2):
            pair = [work[pl.ds((a + o) * 16 + r, 8, stride=PITCH), :] for o in range(2)]
            send[r, 8 * a : 8 * a + 16, :] = jnp.concatenate(pair, axis=0).astype(BF16)


def put_row(received, work, r):
    for a in range(0, 8, 2):
        pair = received[r, 8 * a : 8 * a + 16, :].astype(F32)
        for o in range(2):
            work[pl.ds((a + o) * 16 + r, 8, stride=PITCH), :] = pair[8 * o : 8 * o + 8, :]


def kernel(
    signal_in, taps_in, gate_in, skip_in, left_all, back_all, turn_all, step_all, right_all, undo_all, mid_all,
    out_all,
    signal, taps, gate, skip, out,
    left, back, turn, step, right, undo, mid,
    work, taps_work, send_x, send_g, send_t, ring_t, recv_x, recv_t, recv_g, send_o, recv_o, skips,
    turns, grid_f32, c_high, c_low, spectrum, back_grid, d_high, d_low, y_mine, y_send, y_recv,
    input_sems, table_sems, out_sems,
    sr, rr, sx, rx, st, rt, sg, rg, so, ro, fsx, frx, fst, frt, sy, ry, skip_sems,
):
    shard = lax.axis_index("ctx")
    core = lax.axis_index("core")
    half = lax.div(shard, 16)
    spot = lax.rem(shard, 16)
    first = 16 * core
    other = 16 - first
    mate = {"core": 1 - core}
    row = lax.div(shard, 8)
    col = lax.rem(shard, 8)

    def peer(i):
        return {"ctx": first + i, "core": half}

    def all_peers(body):
        def run(k, carry):
            body(lax.rem(spot + k, 16))
            return carry

        lax.fori_loop(0, 16, run, 0)

    barrier = pltpu.get_barrier_semaphore()

    def others(body):
        def run(i):
            @pl.when(first + i != shard)
            def _():
                body(i)

        all_peers(run)

    def ring(i):
        return {"ctx": row * 8 + i}

    def along_ring(body):
        def run(k, carry):
            body(lax.rem(col + k, 8))
            return carry

        lax.fori_loop(1, 8, run, 0)

    def hello(device):
        pl.semaphore_signal(barrier, inc=1, device_id=device, device_id_type=MESH)

    others(lambda i: hello(peer(i)))
    hello(mate)

    @pl.when(core != half)
    def _():
        along_ring(lambda i: hello(ring(i)))

    def fetch(pairs, sems):
        copies = [pltpu.make_async_copy(a, b, sems.at[i]) for i, (a, b) in enumerate(pairs)]
        for copy in copies:
            copy.start()
        return copies

    inputs = fetch(
        [(taps_in, taps), (signal_in, signal), (gate_in, gate), (skip_in, skip)], input_sems
    )
    copies = fetch(
        [
            (left_all.at[core], left),
            (turn_all.at[core], turn),
            (step_all.at[core], step),
            (right_all, right),
            (mid_all, mid),
            (undo_all, undo),
            (back_all.at[core], back),
        ],
        table_sems,
    )

    inputs[0].wait()
    for j in range(64):
        at = (j % 8) * 8 + j // 8
        taps_work[at : at + 1, :] = taps[:, 128 * j : 128 * j + 128].astype(F32)
    send_t[...] = taps_work[...].astype(BF16)
    inputs[1].wait()
    spread_out(signal, work, send_x)

    pl.semaphore_wait(barrier, jnp.where(core == half, 16, 24))

    def peer_copy(i, src, dst, send_sem, recv_sem):
        return pltpu.make_async_remote_copy(
            src_ref=src, dst_ref=dst, send_sem=send_sem.at[i], recv_sem=recv_sem,
            device_id=peer(i), device_id_type=MESH,
        )

    def ring_copy(i, slot):
        return pltpu.make_async_remote_copy(
            src_ref=send_t, dst_ref=ring_t.at[slot], send_sem=sr.at[i], recv_sem=rr.at[slot],
            device_id=ring(i), device_id_type=MESH,
        )

    def row_copy(block, side):
        i = side * 8 + col
        return pltpu.make_async_remote_copy(
            src_ref=ring_t.at[block], dst_ref=recv_t.at[row * 8 + block], send_sem=st.at[side * 8 + block],
            recv_sem=rt.at[lax.rem(row, 2) * 8 + block], device_id=peer(i), device_id_type=MESH,
        )

    def out_x(i):
        return peer_copy(i, send_x.at[i], recv_x.at[shard], sx, rx.at[spot])

    def out_g(i):
        return peer_copy(i, send_g.at[i], recv_g.at[spot], sg, rg.at[spot])

    def out_o(i):
        return peer_copy(i, send_o.at[i], recv_o.at[spot], so, ro.at[spot])

    def near(i):
        @pl.when(i != lax.rem(col + 4, 8))
        def _():
            ring_copy(i, col).start()

    along_ring(near)
    ring_t[col] = send_t[...]
    before = lax.rem(col + 5, 8)
    far = 8 + lax.rem(col + 4, 8)

    def from_far(body):
        def run(k, carry):
            i = lax.rem(far + k, 16)

            @pl.when(first + i != shard)
            def _():
                body(i)

            return carry

        lax.fori_loop(0, 16, run, 0)

    from_far(lambda i: out_x(i).start())

    @pl.when(core == half)
    def _():
        recv_x[shard] = send_x[spot]

    inputs[2].wait()
    spread_out(gate, work, send_g)
    inputs[3].wait()
    for r in range(16):
        skips[core, r : r + 1, :] = jnp.full((1, 128), skip[r], F32)
    skip_copy = pltpu.make_async_remote_copy(
        src_ref=skips.at[core], dst_ref=skips.at[core], send_sem=skip_sems.at[0],
        recv_sem=skip_sems.at[1], device_id=mate, device_id_type=MESH,
    )
    skip_copy.start()

    def incoming(i, slot, recv_sem):
        return peer_copy(i, send_t, slot, sx, recv_sem.at[i])

    def to_rows(block):
        for side in range(2):

            @pl.when(first + side * 8 + col != shard)
            def _():
                row_copy(block, side).start()

        @pl.when(core == half)
        def _():
            recv_t[row * 8 + block] = ring_t[block]

    to_rows(col)

    def ring_on(i):
        return pltpu.make_async_remote_copy(
            src_ref=ring_t.at[i], dst_ref=ring_t.at[i], send_sem=sr.at[col], recv_sem=rr.at[i],
            device_id=ring(lax.rem(col + 1, 8)), device_id_type=MESH,
        )

    def relay(i):
        ring_copy(i, i).wait_recv()

        @pl.when(i == before)
        def _():
            ring_on(i).start()

        to_rows(i)

    for k in (5, 1, 7, 2, 6, 3, 4):
        relay(lax.rem(col + k, 8))
    others(lambda i: out_g(i).start())

    @pl.when(core == half)
    def _():
        recv_g[spot] = send_g[spot]


    def to_mate(i, ref, slot, send_sem, recv_sem):
        return pltpu.make_async_remote_copy(
            src_ref=ref.at[slot], dst_ref=ref.at[slot], send_sem=send_sem.at[i],
            recv_sem=recv_sem.at[i], device_id=mate, device_id_type=MESH,
        )

    def hand_over(ref, recv_sem, fwd_send, fwd_recv, remote):
        def pass_on(i):
            @pl.when(remote(i))
            def _():
                incoming(i, ref.at[first + i], recv_sem).wait_recv()

            to_mate(i, ref, first + i, fwd_send, fwd_recv).start()

        all_peers(pass_on)

    def take_over(ref, fwd_send, fwd_recv):
        def take(i, carry):
            to_mate(i, ref, other + i, fwd_send, fwd_recv).wait_recv()
            return carry

        lax.fori_loop(0, 16, take, 0)

    for copy in copies:
        copy.wait()
    make_turns(turn, step, turns)

    hand_over(recv_x, rx, fsx, frx, lambda i: first + i != shard)
    hand_over(recv_t, rt, fst, frt, lambda i: lax.div(first + i, 8) != row)
    take_over(recv_x, fsx, frx)
    forward_front(recv_x, left, turns, mid, grid_f32, c_high, c_low)
    spectrum_of(right, c_high, c_low, spectrum)
    take_over(recv_t, fst, frt)
    forward_front(recv_t, left, turns, mid, grid_f32, c_high, c_low)
    middle(right, undo, c_high, c_low, spectrum, back_grid)
    inverse_back(turns, mid, back_grid, d_high, d_low)

    def y_copy(c):
        return pltpu.make_async_remote_copy(
            src_ref=y_send.at[c], dst_ref=y_recv.at[c], send_sem=sy.at[c], recv_sem=ry.at[c],
            device_id=mate, device_id_type=MESH,
        )

    for c in range(4):
        value = inverse_columns(c, back, d_high, d_low)
        y_send[c] = value[128:, :]
        y_mine[c] = value[:128, :]
        y_copy(c).start()
    skip_copy.wait()
    weight = skips[half, pl.ds(spot, 1), :]
    others(lambda i: incoming(i, recv_g.at[i], rg).wait_recv())
    for c in range(4):
        y_copy(c).wait_recv()

    def send_back(i):
        rows = pl.ds(pl.multiple_of(i * 8, 8), 8)
        for c in range(4):
            total = y_mine[c, rows, :] + y_recv[c, rows, :]
            total = jnp.concatenate([total[:, :128], total[:, 128:]], axis=0)
            cut = slice(16 * c, 16 * c + 16)
            direct = recv_x[first + i, cut, :].astype(F32)
            total = recv_g[i, cut, :].astype(F32) * (total + weight * direct)
            send_o[i, cut, :] = total.astype(BF16)

        @pl.when(first + i != shard)
        def _():
            out_o(i).start()

        @pl.when(first + i == shard)
        def _():
            recv_o[spot] = send_o[i]

    all_peers(send_back)

    def place(i):
        @pl.when(first + i != shard)
        def _():
            incoming(i, recv_o.at[i], ro).wait_recv()

        put_row(recv_o, work, i)

    all_peers(place)
    results = []
    for piece in range(4):
        for j in range(16 * piece, 16 * piece + 16):
            at = (j // 8) * PITCH + (j % 8) * 16
            out[piece, :, 128 * (j % 16) : 128 * (j % 16) + 128] = work[at : at + 16, :].astype(BF16)
        cols = slice(2048 * piece, 2048 * piece + 2048)
        results.append(pltpu.make_async_copy(out.at[piece], out_all.at[:, cols], out_sems.at[piece]))
        results[-1].start()

    def sent(i):
        out_x(i).wait_send()
        out_g(i).wait_send()
        out_o(i).wait_send()

    others(sent)

    def ring_sent(i):
        @pl.when(i != lax.rem(col + 4, 8))
        def _():
            ring_copy(i, col).wait_send()

    along_ring(ring_sent)
    ring_on(before).wait_send()

    def rows_sent(block, carry):
        for side in range(2):

            @pl.when(first + side * 8 + col != shard)
            def _():
                row_copy(block, side).wait_send()

        return carry

    lax.fori_loop(0, 8, rows_sent, 0)

    def passed(i, carry):
        to_mate(i, recv_t, first + i, fst, frt).wait_send()
        to_mate(i, recv_x, first + i, fsx, frx).wait_send()
        return carry

    lax.fori_loop(0, 16, passed, 0)
    for c in range(4):
        y_copy(c).wait_send()
    for result in results:
        result.wait()


def local(signal, filter_taps, gate_values, skip_weight):
    held = tables()
    vmem, dma = pltpu.VMEM, pltpu.SemaphoreType.DMA
    apart = pl.BlockSpec(memory_space=pl.ANY)
    scratch = [
        vmem((16, 8192), BF16),
        vmem((1, 8192), BF16),
        vmem((16, 8192), BF16),
        pltpu.SMEM((16,), F32),
        vmem((4, 16, 2048), BF16),
        vmem((2, 256, 256), BF16),
        vmem((2, 256, 256), BF16),
        vmem((2, 128, 128), F32),
        vmem((2, 128, 128), F32),
        vmem((2, 256, 256), BF16),
        vmem((2, 256, 256), BF16),
        vmem((2, 8, 128), F32),
        vmem((8 * PITCH, 128), F32),
        vmem((64, 128), F32),
        vmem((16, 64, 128), BF16),
        vmem((16, 64, 128), BF16),
        vmem((64, 128), BF16),
        vmem((8, 64, 128), BF16),
        vmem((32, 64, 128), BF16),
        vmem((32, 64, 128), BF16),
        vmem((16, 64, 128), BF16),
        vmem((16, 64, 128), BF16),
        vmem((16, 64, 128), BF16),
        vmem((2, 16, 128), F32),
        vmem((2, 8, 128, 128), F32),
        vmem((256, 1024), F32),
        vmem((1024, 256), BF16),
        vmem((1024, 256), BF16),
        vmem((1024, 256), F32),
        vmem((1024, 256), F32),
        vmem((256, 1024), BF16),
        vmem((256, 1024), BF16),
        vmem((4, 128, 256), F32),
        vmem((4, 128, 256), F32),
        vmem((4, 128, 256), F32),
        dma((4,)),
        dma((7,)),
        dma((4,)),
        dma((8,)),
        dma((8,)),
        *[dma((16,)) for _ in range(12)],
        dma((4,)),
        dma((4,)),
        dma((2,)),
    ]
    return pl.pallas_call(
        kernel,
        out_shape=jax.ShapeDtypeStruct(signal.shape, BF16),
        in_specs=[apart] * (4 + len(held)),
        out_specs=apart,
        scratch_shapes=scratch,
        compiler_params=pltpu.CompilerParams(collective_id=0, has_side_effects=True),
        name="hyena",
    )(signal, filter_taps, gate_values, skip_weight, *[jnp.asarray(t) for t in held])


def solution(mesh):
    shards = mesh.shape["ctx"]
    finer = Mesh(mesh.devices.reshape(shards, -1, 2), ("ctx", "x", "core"))
    chan = ("x", "core")
    placed = (P(chan, "ctx"), P(chan, "ctx"), P(chan, "ctx"), P(chan))
    return jax.shard_map(
        local, mesh=finer, in_specs=placed, out_specs=P(chan, "ctx"), check_vma=False
    )
```

```python
import functools

import jax
import jax.numpy as jnp
import ml_dtypes
import numpy as np
from jax import lax
from jax.experimental import pallas as pl
from jax.experimental.pallas import tpu as pltpu
from jax.sharding import Mesh
from jax.sharding import PartitionSpec as P

F32 = jnp.float32
BF16 = jnp.bfloat16
MESH = pl.DeviceIdType.MESH
PITCH = 136
HALF_ROOT = float(np.sqrt(0.5))


def two_parts(table):
    high = table.astype(ml_dtypes.bfloat16)
    low = (table - high.astype(np.float64)).astype(ml_dtypes.bfloat16)
    return np.stack([high, low])


@functools.cache
def tables():
    left, back, turn, step = [], [], [], []
    for core in range(2):
        shift = 0.125 + 0.5 * core
        kl = np.arange(128)[:, None] + shift
        angle = 2.0 * np.pi * np.mod(kl * np.arange(256)[None, :] / 128.0, 1.0)
        forward = np.concatenate([np.cos(angle), -np.sin(angle)], 0)
        left.append(two_parts(forward))
        inverse = np.roll(forward.T, -128 * core, 0)
        back.append(two_parts(inverse))
        angle = 2.0 * np.pi * np.mod(kl * np.arange(128)[None, :] / 131072.0, 1.0)
        turn.append(np.stack([np.cos(angle), -np.sin(angle)]))
        angle = np.broadcast_to(2.0 * np.pi * kl / 1024.0, (128, 128))
        step.append(np.stack([np.cos(angle), -np.sin(angle)]))
    index = np.arange(128)
    angle = 2.0 * np.pi * np.mod(index[:, None] * index[None, :] / 128.0, 1.0)
    cos, sin = np.cos(angle), np.sin(angle)
    right = two_parts(np.block([[cos, -sin], [sin, cos]]))
    undo = two_parts(np.block([[cos, sin], [-sin, cos]]) * 2.0**-18)
    angle = 2.0 * np.pi * np.arange(8)[:, None] * index[None, :] / 1024.0
    mid = np.stack([np.cos(angle), -np.sin(angle)])
    return (
        np.stack(left),
        np.stack(back),
        np.stack(turn).astype(np.float32),
        np.stack(step).astype(np.float32),
        right,
        undo,
        mid.astype(np.float32),
    )


def times(a, b):
    return (a[0] * b[0] - a[1] * b[1], a[0] * b[1] + a[1] * b[0])


def times_conj(a, b):
    return (a[0] * b[0] + a[1] * b[1], a[1] * b[0] - a[0] * b[1])


def plus(a, b):
    return (a[0] + b[0], a[1] + b[1])


def minus(a, b):
    return (a[0] - b[0], a[1] - b[1])


def quarter(a, sign):
    return (-a[1], a[0]) if sign > 0 else (a[1], -a[0])


def dft4(z, sign):
    even, odd = plus(z[0], z[2]), plus(z[1], z[3])
    d_even, d_odd = minus(z[0], z[2]), quarter(minus(z[1], z[3]), sign)
    return [plus(even, odd), plus(d_even, d_odd), minus(even, odd), minus(d_even, d_odd)]


def dft8(z, sign):
    low = [plus(z[j], z[j + 4]) for j in range(4)]
    high = [minus(z[j], z[j + 4]) for j in range(4)]
    h1 = plus(high[1], quarter(high[1], sign))
    h3 = minus(quarter(high[3], sign), high[3])
    high = [
        high[0],
        (h1[0] * HALF_ROOT, h1[1] * HALF_ROOT),
        quarter(high[2], sign),
        (h3[0] * HALF_ROOT, h3[1] * HALF_ROOT),
    ]
    even, odd = dft4(low, sign), dft4(high, sign)
    return [even[0], odd[0], even[1], odd[1], even[2], odd[2], even[3], odd[3]]


def split(value):
    high = value.astype(BF16)
    return high, (value - high.astype(F32)).astype(BF16)


def mm(a, b):
    return jnp.dot(a, b, preferred_element_type=F32)


def make_turns(turn, step, turns):
    def body(q, carry):
        rows = pl.ds(pl.multiple_of(q * 16, 16), 16)
        now = (turn[0, rows, :], turn[1, rows, :])
        by = (step[0, rows, :], step[1, rows, :])
        for a in range(8):
            turns[0, a, rows, :] = now[0]
            turns[1, a, rows, :] = now[1]
            if a < 7:
                now = times(now, by)
        return carry

    lax.fori_loop(0, 8, body, 0)


def first_stage(data, left, grid_f32):
    for c in range(4):
        tile = data[:, 16 * c : 16 * c + 16, :].astype(F32)
        block = jnp.concatenate(
            [tile[:, :8, :].reshape(256, 128), tile[:, 8:, :].reshape(256, 128)], axis=1
        ).astype(BF16)
        grid_f32[:, 256 * c : 256 * c + 256] = mm(left[0], block) + mm(left[1], block)


def second_stage(at, turns, mid, grid_f32):
    rows = slice(at, at + 16)
    z = []
    for a in range(8):
        cols = slice(128 * a, 128 * a + 128)
        value = (grid_f32[rows, cols], grid_f32[at + 128 : at + 144, cols])
        z.append(times(value, (turns[0, a, rows, :], turns[1, a, rows, :])))
    z = dft8(z, -1)
    for ka in range(1, 8):
        z[ka] = times(z[ka], (mid[0, ka : ka + 1, :], mid[1, ka : ka + 1, :]))
    return split(jnp.concatenate([jnp.concatenate(v, axis=1) for v in z], axis=0))


def transform_rows(m, right, turns, mid, grid_f32):
    parts = [second_stage(32 * m + 16 * o, turns, mid, grid_f32) for o in range(2)]
    high = jnp.concatenate([p[0] for p in parts], axis=0)
    low = jnp.concatenate([p[1] for p in parts], axis=0)
    return mm(high, right[0]) + mm(low, right[0]) + mm(high, right[1])


def spectrum_of(data, left, right, turns, mid, grid_f32, spectrum):
    first_stage(data, left, grid_f32)
    for m in range(4):
        spectrum[256 * m : 256 * m + 256, :] = transform_rows(m, right, turns, mid, grid_f32)


def middle(data, left, right, undo, turns, mid, grid_f32, spectrum, d_high, d_low):
    first_stage(data, left, grid_f32)
    for m in range(4):
        value = transform_rows(m, right, turns, mid, grid_f32)
        known = spectrum[256 * m : 256 * m + 256, :]
        re, im = times((value[:, :128], value[:, 128:]), (known[:, :128], known[:, 128:]))
        high, low = split(jnp.concatenate([re, im], axis=1))
        value = mm(high, undo[0]) + mm(low, undo[0]) + mm(high, undo[1])
        for o in range(2):
            at = 32 * m + 16 * o
            z = []
            for ka in range(8):
                rows = slice(128 * o + 16 * ka, 128 * o + 16 * ka + 16)
                z.append((value[rows, :128], value[rows, 128:]))
                if ka:
                    z[ka] = times_conj(z[ka], (mid[0, ka : ka + 1, :], mid[1, ka : ka + 1, :]))
            z = dft8(z, 1)
            for a in range(8):
                rows = slice(at, at + 16)
                back = times_conj(z[a], (turns[0, a, rows, :], turns[1, a, rows, :]))
                cols = slice(128 * a, 128 * a + 128)
                for part in range(2):
                    rows = slice(at + 128 * part, at + 128 * part + 16)
                    d_high[rows, cols], d_low[rows, cols] = split(back[part])


def inverse_columns(c, back, d_high, d_low):
    cols = slice(256 * c, 256 * c + 256)
    high, low = d_high[:, cols], d_low[:, cols]
    return mm(back[0], high) + mm(back[0], low) + mm(back[1], high)


def spread_out(rows_ref, work, send):
    for j in range(64):
        at = (j // 8) * PITCH + (j % 8) * 16
        work[at : at + 16, :] = rows_ref[:, 128 * j : 128 * j + 128].astype(F32)
    for r in range(16):
        for a in range(0, 8, 2):
            pair = [work[pl.ds((a + o) * 16 + r, 8, stride=PITCH), :] for o in range(2)]
            send[r, 8 * a : 8 * a + 16, :] = jnp.concatenate(pair, axis=0).astype(BF16)


def put_row(received, work, r):
    for a in range(0, 8, 2):
        pair = received[r, 8 * a : 8 * a + 16, :].astype(F32)
        for o in range(2):
            work[pl.ds((a + o) * 16 + r, 8, stride=PITCH), :] = pair[8 * o : 8 * o + 8, :]


def kernel(
    signal_in, taps_in, gate_in, skip_in, left_all, back_all, turn_all, step_all, right_all, undo_all, mid_all,
    out_all,
    signal, taps, gate, skip, out,
    left, back, turn, step, right, undo, mid,
    work, taps_work, send_x, send_g, send_t, ring_t, recv_x, recv_t, recv_g, send_o, recv_o, skips,
    turns, grid_f32, spectrum, d_high, d_low, y_mine, y_send, y_recv,
    input_sems, table_sems, out_sems,
    sr, rr, sx, rx, st, rt, sg, rg, so, ro, fsx, frx, fst, frt, sy, ry, skip_sems,
):
    shard = lax.axis_index("ctx")
    core = lax.axis_index("core")
    half = lax.div(shard, 16)
    spot = lax.rem(shard, 16)
    first = 16 * core
    other = 16 - first
    mate = {"core": 1 - core}
    row = lax.div(shard, 8)
    col = lax.rem(shard, 8)

    def peer(i):
        return {"ctx": first + i, "core": half}

    def all_peers(body):
        def run(k, carry):
            body(lax.rem(spot + k, 16))
            return carry

        lax.fori_loop(0, 16, run, 0)

    barrier = pltpu.get_barrier_semaphore()

    def others(body):
        def run(i):
            @pl.when(first + i != shard)
            def _():
                body(i)

        all_peers(run)

    def ring(i):
        return {"ctx": row * 8 + i}

    def along_ring(body):
        def run(k, carry):
            body(lax.rem(col + k, 8))
            return carry

        lax.fori_loop(1, 8, run, 0)

    def hello(device):
        pl.semaphore_signal(barrier, inc=1, device_id=device, device_id_type=MESH)

    others(lambda i: hello(peer(i)))
    hello(mate)

    @pl.when(core != half)
    def _():
        along_ring(lambda i: hello(ring(i)))

    def fetch(pairs, sems):
        copies = [pltpu.make_async_copy(a, b, sems.at[i]) for i, (a, b) in enumerate(pairs)]
        for copy in copies:
            copy.start()
        return copies

    inputs = fetch(
        [(taps_in, taps), (signal_in, signal), (gate_in, gate), (skip_in, skip)], input_sems
    )
    copies = fetch(
        [
            (left_all.at[core], left),
            (turn_all.at[core], turn),
            (step_all.at[core], step),
            (right_all, right),
            (mid_all, mid),
            (undo_all, undo),
            (back_all.at[core], back),
        ],
        table_sems,
    )

    inputs[0].wait()
    for j in range(64):
        at = (j % 8) * 8 + j // 8
        taps_work[at : at + 1, :] = taps[:, 128 * j : 128 * j + 128].astype(F32)
    send_t[...] = taps_work[...].astype(BF16)
    inputs[1].wait()
    spread_out(signal, work, send_x)

    pl.semaphore_wait(barrier, jnp.where(core == half, 16, 24))

    def peer_copy(i, src, dst, send_sem, recv_sem):
        return pltpu.make_async_remote_copy(
            src_ref=src, dst_ref=dst, send_sem=send_sem.at[i], recv_sem=recv_sem,
            device_id=peer(i), device_id_type=MESH,
        )

    def ring_copy(i, slot):
        return pltpu.make_async_remote_copy(
            src_ref=send_t, dst_ref=ring_t.at[slot], send_sem=sr.at[i], recv_sem=rr.at[slot],
            device_id=ring(i), device_id_type=MESH,
        )

    def row_copy(block, side):
        i = side * 8 + col
        return pltpu.make_async_remote_copy(
            src_ref=ring_t.at[block], dst_ref=recv_t.at[row * 8 + block], send_sem=st.at[side * 8 + block],
            recv_sem=rt.at[lax.rem(row, 2) * 8 + block], device_id=peer(i), device_id_type=MESH,
        )

    def out_x(i):
        return peer_copy(i, send_x.at[i], recv_x.at[shard], sx, rx.at[spot])

    def out_g(i):
        return peer_copy(i, send_g.at[i], recv_g.at[spot], sg, rg.at[spot])

    def out_o(i):
        return peer_copy(i, send_o.at[i], recv_o.at[spot], so, ro.at[spot])

    def near(i):
        @pl.when(i != lax.rem(col + 4, 8))
        def _():
            ring_copy(i, col).start()

    along_ring(near)
    ring_t[col] = send_t[...]
    before = lax.rem(col + 5, 8)
    far = 8 + lax.rem(col + 4, 8)

    def in_order(body):
        def run(k, carry):
            i = lax.rem(far + k, 16)
            body(i)
            return carry

        lax.fori_loop(0, 16, run, 0)

    def from_far(body):
        def run(i):
            @pl.when(first + i != shard)
            def _():
                body(i)

        in_order(run)

    from_far(lambda i: out_x(i).start())

    @pl.when(core == half)
    def _():
        recv_x[shard] = send_x[spot]

    inputs[2].wait()
    spread_out(gate, work, send_g)
    inputs[3].wait()
    for r in range(16):
        skips[core, r : r + 1, :] = jnp.full((1, 128), skip[r], F32)
    skip_copy = pltpu.make_async_remote_copy(
        src_ref=skips.at[core], dst_ref=skips.at[core], send_sem=skip_sems.at[0],
        recv_sem=skip_sems.at[1], device_id=mate, device_id_type=MESH,
    )
    skip_copy.start()

    def incoming(i, slot, recv_sem):
        return peer_copy(i, send_t, slot, sx, recv_sem.at[i])

    def to_rows(block):
        for side in range(2):

            @pl.when(first + side * 8 + col != shard)
            def _():
                row_copy(block, side).start()

        @pl.when(core == half)
        def _():
            recv_t[row * 8 + block] = ring_t[block]

    to_rows(col)

    def ring_on(i):
        return pltpu.make_async_remote_copy(
            src_ref=ring_t.at[i], dst_ref=ring_t.at[i], send_sem=sr.at[col], recv_sem=rr.at[i],
            device_id=ring(lax.rem(col + 1, 8)), device_id_type=MESH,
        )

    def relay(i):
        ring_copy(i, i).wait_recv()

        @pl.when(i == before)
        def _():
            ring_on(i).start()

        to_rows(i)

    for k in (5, 1, 7, 2, 6, 3, 4):
        relay(lax.rem(col + k, 8))
    others(lambda i: out_g(i).start())

    @pl.when(core == half)
    def _():
        recv_g[spot] = send_g[spot]


    def to_mate(i, ref, slot, send_sem, recv_sem):
        return pltpu.make_async_remote_copy(
            src_ref=ref.at[slot], dst_ref=ref.at[slot], send_sem=send_sem.at[i],
            recv_sem=recv_sem.at[i], device_id=mate, device_id_type=MESH,
        )

    def hand_over(ref, recv_sem, fwd_send, fwd_recv, remote):
        def pass_on(i):
            @pl.when(remote(i))
            def _():
                incoming(i, ref.at[first + i], recv_sem).wait_recv()

            to_mate(i, ref, first + i, fwd_send, fwd_recv).start()

        all_peers(pass_on)

    def take_over(ref, fwd_send, fwd_recv):
        def take(i, carry):
            to_mate(i, ref, other + i, fwd_send, fwd_recv).wait_recv()
            return carry

        lax.fori_loop(0, 16, take, 0)

    for copy in copies:
        copy.wait()
    make_turns(turn, step, turns)

    hand_over(recv_x, rx, fsx, frx, lambda i: first + i != shard)
    hand_over(recv_t, rt, fst, frt, lambda i: lax.div(first + i, 8) != row)
    take_over(recv_x, fsx, frx)
    spectrum_of(recv_x, left, right, turns, mid, grid_f32, spectrum)
    take_over(recv_t, fst, frt)
    middle(recv_t, left, right, undo, turns, mid, grid_f32, spectrum, d_high, d_low)

    def y_copy(c):
        return pltpu.make_async_remote_copy(
            src_ref=y_send.at[c], dst_ref=y_recv.at[c], send_sem=sy.at[c], recv_sem=ry.at[c],
            device_id=mate, device_id_type=MESH,
        )

    for c in range(4):
        value = inverse_columns(c, back, d_high, d_low)
        y_send[c] = value[128:, :]
        y_mine[c] = value[:128, :]
        y_copy(c).start()
    skip_copy.wait()
    weight = skips[half, pl.ds(spot, 1), :]
    others(lambda i: incoming(i, recv_g.at[i], rg).wait_recv())
    for c in range(4):
        y_copy(c).wait_recv()

    def send_back(i):
        rows = pl.ds(pl.multiple_of(i * 8, 8), 8)
        for c in range(4):
            total = y_mine[c, rows, :] + y_recv[c, rows, :]
            total = jnp.concatenate([total[:, :128], total[:, 128:]], axis=0)
            cut = slice(16 * c, 16 * c + 16)
            direct = recv_x[first + i, cut, :].astype(F32)
            total = recv_g[i, cut, :].astype(F32) * (total + weight * direct)
            send_o[i, cut, :] = total.astype(BF16)

        @pl.when(first + i != shard)
        def _():
            out_o(i).start()

        @pl.when(first + i == shard)
        def _():
            recv_o[spot] = send_o[i]

    in_order(send_back)

    def place(i):
        @pl.when(first + i != shard)
        def _():
            incoming(i, recv_o.at[i], ro).wait_recv()

        put_row(recv_o, work, i)

    all_peers(place)
    results = []
    for piece in range(4):
        for j in range(16 * piece, 16 * piece + 16):
            at = (j // 8) * PITCH + (j % 8) * 16
            out[piece, :, 128 * (j % 16) : 128 * (j % 16) + 128] = work[at : at + 16, :].astype(BF16)
        cols = slice(2048 * piece, 2048 * piece + 2048)
        results.append(pltpu.make_async_copy(out.at[piece], out_all.at[:, cols], out_sems.at[piece]))
        results[-1].start()

    def sent(i):
        out_x(i).wait_send()
        out_g(i).wait_send()
        out_o(i).wait_send()

    others(sent)

    def ring_sent(i):
        @pl.when(i != lax.rem(col + 4, 8))
        def _():
            ring_copy(i, col).wait_send()

    along_ring(ring_sent)
    ring_on(before).wait_send()

    def rows_sent(block, carry):
        for side in range(2):

            @pl.when(first + side * 8 + col != shard)
            def _():
                row_copy(block, side).wait_send()

        return carry

    lax.fori_loop(0, 8, rows_sent, 0)

    def passed(i, carry):
        to_mate(i, recv_t, first + i, fst, frt).wait_send()
        to_mate(i, recv_x, first + i, fsx, frx).wait_send()
        return carry

    lax.fori_loop(0, 16, passed, 0)
    for c in range(4):
        y_copy(c).wait_send()
    for result in results:
        result.wait()


def local(signal, filter_taps, gate_values, skip_weight):
    held = tables()
    vmem, dma = pltpu.VMEM, pltpu.SemaphoreType.DMA
    apart = pl.BlockSpec(memory_space=pl.ANY)
    scratch = [
        vmem((16, 8192), BF16),
        vmem((1, 8192), BF16),
        vmem((16, 8192), BF16),
        pltpu.SMEM((16,), F32),
        vmem((4, 16, 2048), BF16),
        vmem((2, 256, 256), BF16),
        vmem((2, 256, 256), BF16),
        vmem((2, 128, 128), F32),
        vmem((2, 128, 128), F32),
        vmem((2, 256, 256), BF16),
        vmem((2, 256, 256), BF16),
        vmem((2, 8, 128), F32),
        vmem((8 * PITCH, 128), F32),
        vmem((64, 128), F32),
        vmem((16, 64, 128), BF16),
        vmem((16, 64, 128), BF16),
        vmem((64, 128), BF16),
        vmem((8, 64, 128), BF16),
        vmem((32, 64, 128), BF16),
        vmem((32, 64, 128), BF16),
        vmem((16, 64, 128), BF16),
        vmem((16, 64, 128), BF16),
        vmem((16, 64, 128), BF16),
        vmem((2, 16, 128), F32),
        vmem((2, 8, 128, 128), F32),
        vmem((256, 1024), F32),
        vmem((1024, 256), F32),
        vmem((256, 1024), BF16),
        vmem((256, 1024), BF16),
        vmem((4, 128, 256), F32),
        vmem((4, 128, 256), F32),
        vmem((4, 128, 256), F32),
        dma((4,)),
        dma((7,)),
        dma((4,)),
        dma((8,)),
        dma((8,)),
        *[dma((16,)) for _ in range(12)],
        dma((4,)),
        dma((4,)),
        dma((2,)),
    ]
    return pl.pallas_call(
        kernel,
        out_shape=jax.ShapeDtypeStruct(signal.shape, BF16),
        in_specs=[apart] * (4 + len(held)),
        out_specs=apart,
        scratch_shapes=scratch,
        compiler_params=pltpu.CompilerParams(collective_id=0, has_side_effects=True),
        name="hyena",
    )(signal, filter_taps, gate_values, skip_weight, *[jnp.asarray(t) for t in held])


def solution(mesh):
    shards = mesh.shape["ctx"]
    finer = Mesh(mesh.devices.reshape(shards, -1, 2), ("ctx", "x", "core"))
    chan = ("x", "core")
    placed = (P(chan, "ctx"), P(chan, "ctx"), P(chan, "ctx"), P(chan))
    return jax.shard_map(
        local, mesh=finer, in_specs=placed, out_specs=P(chan, "ctx"), check_vma=False
    )
```

```python
import functools

import jax
import jax.numpy as jnp
import ml_dtypes
import numpy as np
from jax import lax
from jax.experimental import pallas as pl
from jax.experimental.pallas import tpu as pltpu
from jax.sharding import Mesh
from jax.sharding import PartitionSpec as P

F32 = jnp.float32
BF16 = jnp.bfloat16
MESH = pl.DeviceIdType.MESH
PITCH = 136
HALF_ROOT = float(np.sqrt(0.5))


def two_parts(table):
    high = table.astype(ml_dtypes.bfloat16)
    low = (table - high.astype(np.float64)).astype(ml_dtypes.bfloat16)
    return np.stack([high, low])


@functools.cache
def tables():
    left, back, turn, step = [], [], [], []
    for core in range(2):
        shift = 0.125 + 0.5 * core
        kl = np.arange(128)[:, None] + shift
        angle = 2.0 * np.pi * np.mod(kl * np.arange(256)[None, :] / 128.0, 1.0)
        forward = np.concatenate([np.cos(angle), -np.sin(angle)], 0)
        left.append(two_parts(forward))
        inverse = np.roll(forward.T, -128 * core, 0)
        back.append(two_parts(inverse))
        angle = 2.0 * np.pi * np.mod(kl * np.arange(128)[None, :] / 131072.0, 1.0)
        turn.append(np.stack([np.cos(angle), -np.sin(angle)]))
        angle = np.broadcast_to(2.0 * np.pi * kl / 1024.0, (128, 128))
        step.append(np.stack([np.cos(angle), -np.sin(angle)]))
    index = np.arange(128)
    angle = 2.0 * np.pi * np.mod(index[:, None] * index[None, :] / 128.0, 1.0)
    cos, sin = np.cos(angle), np.sin(angle)
    right = two_parts(np.block([[cos, -sin], [sin, cos]]))
    undo = two_parts(np.block([[cos, sin], [-sin, cos]]) * 2.0**-18)
    angle = 2.0 * np.pi * np.arange(8)[:, None] * index[None, :] / 1024.0
    mid = np.stack([np.cos(angle), -np.sin(angle)])
    return (
        np.stack(left),
        np.stack(back),
        np.stack(turn).astype(np.float32),
        np.stack(step).astype(np.float32),
        right,
        undo,
        mid.astype(np.float32),
    )


def times(a, b):
    return (a[0] * b[0] - a[1] * b[1], a[0] * b[1] + a[1] * b[0])


def times_conj(a, b):
    return (a[0] * b[0] + a[1] * b[1], a[1] * b[0] - a[0] * b[1])


def plus(a, b):
    return (a[0] + b[0], a[1] + b[1])


def minus(a, b):
    return (a[0] - b[0], a[1] - b[1])


def quarter(a, sign):
    return (-a[1], a[0]) if sign > 0 else (a[1], -a[0])


def dft4(z, sign):
    even, odd = plus(z[0], z[2]), plus(z[1], z[3])
    d_even, d_odd = minus(z[0], z[2]), quarter(minus(z[1], z[3]), sign)
    return [plus(even, odd), plus(d_even, d_odd), minus(even, odd), minus(d_even, d_odd)]


def dft8(z, sign):
    low = [plus(z[j], z[j + 4]) for j in range(4)]
    high = [minus(z[j], z[j + 4]) for j in range(4)]
    h1 = plus(high[1], quarter(high[1], sign))
    h3 = minus(quarter(high[3], sign), high[3])
    high = [
        high[0],
        (h1[0] * HALF_ROOT, h1[1] * HALF_ROOT),
        quarter(high[2], sign),
        (h3[0] * HALF_ROOT, h3[1] * HALF_ROOT),
    ]
    even, odd = dft4(low, sign), dft4(high, sign)
    return [even[0], odd[0], even[1], odd[1], even[2], odd[2], even[3], odd[3]]


def split(value):
    high = value.astype(BF16)
    return high, (value - high.astype(F32)).astype(BF16)


def mm(a, b):
    return jnp.dot(a, b, preferred_element_type=F32)


def make_turns(turn, step, turns):
    def body(q, carry):
        rows = pl.ds(pl.multiple_of(q * 16, 16), 16)
        now = (turn[0, rows, :], turn[1, rows, :])
        by = (step[0, rows, :], step[1, rows, :])
        for a in range(8):
            turns[0, a, rows, :] = now[0]
            turns[1, a, rows, :] = now[1]
            if a < 7:
                now = times(now, by)
        return carry

    lax.fori_loop(0, 8, body, 0)


def first_stage(data, left, grid_f32):
    for c in range(4):
        tile = data[:, 16 * c : 16 * c + 16, :].astype(F32)
        block = jnp.concatenate(
            [tile[:, :8, :].reshape(256, 128), tile[:, 8:, :].reshape(256, 128)], axis=1
        ).astype(BF16)
        grid_f32[:, 256 * c : 256 * c + 256] = mm(left[0], block) + mm(left[1], block)


def second_stage(at, turns, mid, grid_f32):
    rows = slice(at, at + 16)
    z = []
    for a in range(8):
        cols = slice(128 * a, 128 * a + 128)
        value = (grid_f32[rows, cols], grid_f32[at + 128 : at + 144, cols])
        z.append(times(value, (turns[0, a, rows, :], turns[1, a, rows, :])))
    z = dft8(z, -1)
    for ka in range(1, 8):
        z[ka] = times(z[ka], (mid[0, ka : ka + 1, :], mid[1, ka : ka + 1, :]))
    return split(jnp.concatenate([jnp.concatenate(v, axis=1) for v in z], axis=0))


def transform_rows(m, right, turns, mid, grid_f32):
    parts = [second_stage(32 * m + 16 * o, turns, mid, grid_f32) for o in range(2)]
    high = jnp.concatenate([p[0] for p in parts], axis=0)
    low = jnp.concatenate([p[1] for p in parts], axis=0)
    return mm(high, right[0]) + mm(low, right[0]) + mm(high, right[1])


def spectrum_of(data, left, right, turns, mid, grid_f32, spectrum):
    first_stage(data, left, grid_f32)
    for m in range(4):
        spectrum[256 * m : 256 * m + 256, :] = transform_rows(m, right, turns, mid, grid_f32)


def middle(data, left, right, undo, turns, mid, grid_f32, spectrum, d_high, d_low):
    first_stage(data, left, grid_f32)
    for m in range(4):
        value = transform_rows(m, right, turns, mid, grid_f32)
        known = spectrum[256 * m : 256 * m + 256, :]
        re, im = times((value[:, :128], value[:, 128:]), (known[:, :128], known[:, 128:]))
        high, low = split(jnp.concatenate([re, im], axis=1))
        value = mm(high, undo[0]) + mm(low, undo[0]) + mm(high, undo[1])
        for o in range(2):
            at = 32 * m + 16 * o
            z = []
            for ka in range(8):
                rows = slice(128 * o + 16 * ka, 128 * o + 16 * ka + 16)
                z.append((value[rows, :128], value[rows, 128:]))
                if ka:
                    z[ka] = times_conj(z[ka], (mid[0, ka : ka + 1, :], mid[1, ka : ka + 1, :]))
            z = dft8(z, 1)
            for a in range(8):
                rows = slice(at, at + 16)
                back = times_conj(z[a], (turns[0, a, rows, :], turns[1, a, rows, :]))
                cols = slice(128 * a, 128 * a + 128)
                for part in range(2):
                    rows = slice(at + 128 * part, at + 128 * part + 16)
                    d_high[rows, cols], d_low[rows, cols] = split(back[part])


def inverse_columns(c, back, d_high, d_low):
    cols = slice(256 * c, 256 * c + 256)
    high, low = d_high[:, cols], d_low[:, cols]
    return mm(back[0], high) + mm(back[0], low) + mm(back[1], high)


def spread_out(rows_ref, work, send):
    for j in range(64):
        at = (j // 8) * PITCH + (j % 8) * 16
        work[at : at + 16, :] = rows_ref[:, 128 * j : 128 * j + 128].astype(F32)
    for r in range(16):
        for a in range(0, 8, 2):
            pair = [work[pl.ds((a + o) * 16 + r, 8, stride=PITCH), :] for o in range(2)]
            send[r, 8 * a : 8 * a + 16, :] = jnp.concatenate(pair, axis=0).astype(BF16)


def put_row(received, work, r):
    for a in range(0, 8, 2):
        pair = received[r, 8 * a : 8 * a + 16, :].astype(F32)
        for o in range(2):
            work[pl.ds((a + o) * 16 + r, 8, stride=PITCH), :] = pair[8 * o : 8 * o + 8, :]


def kernel(
    signal_in, taps_in, gate_in, skip_in, left_all, back_all, turn_all, step_all, right_all, undo_all, mid_all,
    out,
    signal, taps, gate, skip,
    left, back, turn, step, right, undo, mid,
    work, taps_work, send_x, send_g, send_t, ring_t, recv_x, recv_t, recv_g, send_o, recv_o, skips,
    turns, grid_f32, spectrum, d_high, d_low, y_mine, y_send, y_recv,
    input_sems, table_sems,
    sr, rr, sx, rx, st, rt, sg, rg, so, ro, fsx, frx, fst, frt, sy, ry, skip_sems,
):
    shard = lax.axis_index("ctx")
    core = lax.axis_index("core")
    half = lax.div(shard, 16)
    spot = lax.rem(shard, 16)
    first = 16 * core
    other = 16 - first
    mate = {"core": 1 - core}
    row = lax.div(shard, 8)
    col = lax.rem(shard, 8)

    def peer(i):
        return {"ctx": first + i, "core": half}

    def all_peers(body):
        def run(k, carry):
            body(lax.rem(spot + k, 16))
            return carry

        lax.fori_loop(0, 16, run, 0)

    barrier = pltpu.get_barrier_semaphore()

    def others(body):
        def run(i):
            @pl.when(first + i != shard)
            def _():
                body(i)

        all_peers(run)

    def ring(i):
        return {"ctx": row * 8 + i}

    def along_ring(body):
        def run(k, carry):
            body(lax.rem(col + k, 8))
            return carry

        lax.fori_loop(1, 8, run, 0)

    def hello(device):
        pl.semaphore_signal(barrier, inc=1, device_id=device, device_id_type=MESH)

    others(lambda i: hello(peer(i)))
    hello(mate)

    @pl.when(core != half)
    def _():
        along_ring(lambda i: hello(ring(i)))

    def fetch(pairs, sems):
        copies = [pltpu.make_async_copy(a, b, sems.at[i]) for i, (a, b) in enumerate(pairs)]
        for copy in copies:
            copy.start()
        return copies

    inputs = fetch(
        [(taps_in, taps), (signal_in, signal), (gate_in, gate), (skip_in, skip)], input_sems
    )
    copies = fetch(
        [
            (left_all.at[core], left),
            (turn_all.at[core], turn),
            (step_all.at[core], step),
            (right_all, right),
            (mid_all, mid),
            (undo_all, undo),
            (back_all.at[core], back),
        ],
        table_sems,
    )

    inputs[0].wait()
    for j in range(64):
        at = (j % 8) * 8 + j // 8
        taps_work[at : at + 1, :] = taps[:, 128 * j : 128 * j + 128].astype(F32)
    send_t[...] = taps_work[...].astype(BF16)
    inputs[1].wait()
    spread_out(signal, work, send_x)

    pl.semaphore_wait(barrier, jnp.where(core == half, 16, 24))

    def peer_copy(i, src, dst, send_sem, recv_sem):
        return pltpu.make_async_remote_copy(
            src_ref=src, dst_ref=dst, send_sem=send_sem.at[i], recv_sem=recv_sem,
            device_id=peer(i), device_id_type=MESH,
        )

    def ring_copy(i, slot):
        return pltpu.make_async_remote_copy(
            src_ref=send_t, dst_ref=ring_t.at[slot], send_sem=sr.at[i], recv_sem=rr.at[slot],
            device_id=ring(i), device_id_type=MESH,
        )

    def row_copy(block, side):
        i = side * 8 + col
        return pltpu.make_async_remote_copy(
            src_ref=ring_t.at[block], dst_ref=recv_t.at[row * 8 + block], send_sem=st.at[side * 8 + block],
            recv_sem=rt.at[lax.rem(row, 2) * 8 + block], device_id=peer(i), device_id_type=MESH,
        )

    def out_x(i):
        return peer_copy(i, send_x.at[i], recv_x.at[shard], sx, rx.at[spot])

    def out_g(i):
        return peer_copy(i, send_g.at[i], recv_g.at[spot], sg, rg.at[spot])

    def out_o(i):
        return peer_copy(i, send_o.at[i], recv_o.at[spot], so, ro.at[spot])

    def near(i):
        @pl.when(i != lax.rem(col + 4, 8))
        def _():
            ring_copy(i, col).start()

    along_ring(near)
    ring_t[col] = send_t[...]
    before = lax.rem(col + 5, 8)
    far = 8 + lax.rem(col + 4, 8)

    def in_order(body):
        def run(k, carry):
            i = lax.rem(far + k, 16)
            body(i)
            return carry

        lax.fori_loop(0, 16, run, 0)

    def from_far(body):
        def run(i):
            @pl.when(first + i != shard)
            def _():
                body(i)

        in_order(run)

    from_far(lambda i: out_x(i).start())

    @pl.when(core == half)
    def _():
        recv_x[shard] = send_x[spot]

    inputs[2].wait()
    spread_out(gate, work, send_g)
    inputs[3].wait()
    for r in range(16):
        skips[core, r : r + 1, :] = jnp.full((1, 128), skip[r], F32)
    skip_copy = pltpu.make_async_remote_copy(
        src_ref=skips.at[core], dst_ref=skips.at[core], send_sem=skip_sems.at[0],
        recv_sem=skip_sems.at[1], device_id=mate, device_id_type=MESH,
    )
    skip_copy.start()

    def incoming(i, slot, recv_sem):
        return peer_copy(i, send_t, slot, sx, recv_sem.at[i])

    def to_rows(block):
        for side in range(2):

            @pl.when(first + side * 8 + col != shard)
            def _():
                row_copy(block, side).start()

        @pl.when(core == half)
        def _():
            recv_t[row * 8 + block] = ring_t[block]

    to_rows(col)

    def ring_on(i):
        return pltpu.make_async_remote_copy(
            src_ref=ring_t.at[i], dst_ref=ring_t.at[i], send_sem=sr.at[col], recv_sem=rr.at[i],
            device_id=ring(lax.rem(col + 1, 8)), device_id_type=MESH,
        )

    def relay(i):
        ring_copy(i, i).wait_recv()

        @pl.when(i == before)
        def _():
            ring_on(i).start()

        to_rows(i)

    for k in (5, 1, 7, 2, 6, 3, 4):
        relay(lax.rem(col + k, 8))
    others(lambda i: out_g(i).start())

    @pl.when(core == half)
    def _():
        recv_g[spot] = send_g[spot]


    def to_mate(i, ref, slot, send_sem, recv_sem):
        return pltpu.make_async_remote_copy(
            src_ref=ref.at[slot], dst_ref=ref.at[slot], send_sem=send_sem.at[i],
            recv_sem=recv_sem.at[i], device_id=mate, device_id_type=MESH,
        )

    def hand_over(ref, recv_sem, fwd_send, fwd_recv, remote):
        def pass_on(i):
            @pl.when(remote(i))
            def _():
                incoming(i, ref.at[first + i], recv_sem).wait_recv()

            to_mate(i, ref, first + i, fwd_send, fwd_recv).start()

        all_peers(pass_on)

    def take_over(ref, fwd_send, fwd_recv):
        def take(i, carry):
            to_mate(i, ref, other + i, fwd_send, fwd_recv).wait_recv()
            return carry

        lax.fori_loop(0, 16, take, 0)

    for copy in copies:
        copy.wait()
    make_turns(turn, step, turns)

    hand_over(recv_x, rx, fsx, frx, lambda i: first + i != shard)
    hand_over(recv_t, rt, fst, frt, lambda i: lax.div(first + i, 8) != row)
    take_over(recv_x, fsx, frx)
    spectrum_of(recv_x, left, right, turns, mid, grid_f32, spectrum)
    take_over(recv_t, fst, frt)
    middle(recv_t, left, right, undo, turns, mid, grid_f32, spectrum, d_high, d_low)

    def y_copy(c):
        return pltpu.make_async_remote_copy(
            src_ref=y_send.at[c], dst_ref=y_recv.at[c], send_sem=sy.at[c], recv_sem=ry.at[c],
            device_id=mate, device_id_type=MESH,
        )

    for c in range(4):
        value = inverse_columns(c, back, d_high, d_low)
        y_send[c] = value[128:, :]
        y_mine[c] = value[:128, :]
        y_copy(c).start()
    skip_copy.wait()
    weight = skips[half, pl.ds(spot, 1), :]
    others(lambda i: incoming(i, recv_g.at[i], rg).wait_recv())
    for c in range(4):
        y_copy(c).wait_recv()

    def send_back(i):
        rows = pl.ds(pl.multiple_of(i * 8, 8), 8)
        for c in range(4):
            total = y_mine[c, rows, :] + y_recv[c, rows, :]
            total = jnp.concatenate([total[:, :128], total[:, 128:]], axis=0)
            cut = slice(16 * c, 16 * c + 16)
            direct = recv_x[first + i, cut, :].astype(F32)
            total = recv_g[i, cut, :].astype(F32) * (total + weight * direct)
            send_o[i, cut, :] = total.astype(BF16)

        @pl.when(first + i != shard)
        def _():
            out_o(i).start()

        @pl.when(first + i == shard)
        def _():
            recv_o[spot] = send_o[i]

    in_order(send_back)

    def place(i):
        @pl.when(first + i != shard)
        def _():
            incoming(i, recv_o.at[i], ro).wait_recv()

        put_row(recv_o, work, i)

    all_peers(place)
    for j in range(64):
        at = (j // 8) * PITCH + (j % 8) * 16
        out[:, 128 * j : 128 * j + 128] = work[at : at + 16, :].astype(BF16)

    def sent(i):
        out_x(i).wait_send()
        out_g(i).wait_send()
        out_o(i).wait_send()

    others(sent)

    def ring_sent(i):
        @pl.when(i != lax.rem(col + 4, 8))
        def _():
            ring_copy(i, col).wait_send()

    along_ring(ring_sent)
    ring_on(before).wait_send()

    def rows_sent(block, carry):
        for side in range(2):

            @pl.when(first + side * 8 + col != shard)
            def _():
                row_copy(block, side).wait_send()

        return carry

    lax.fori_loop(0, 8, rows_sent, 0)

    def passed(i, carry):
        to_mate(i, recv_t, first + i, fst, frt).wait_send()
        to_mate(i, recv_x, first + i, fsx, frx).wait_send()
        return carry

    lax.fori_loop(0, 16, passed, 0)
    for c in range(4):
        y_copy(c).wait_send()


def local(signal, filter_taps, gate_values, skip_weight):
    held = tables()
    vmem, dma = pltpu.VMEM, pltpu.SemaphoreType.DMA
    apart = pl.BlockSpec(memory_space=pl.ANY)
    scratch = [
        vmem((16, 8192), BF16),
        vmem((1, 8192), BF16),
        vmem((16, 8192), BF16),
        pltpu.SMEM((16,), F32),
        vmem((2, 256, 256), BF16),
        vmem((2, 256, 256), BF16),
        vmem((2, 128, 128), F32),
        vmem((2, 128, 128), F32),
        vmem((2, 256, 256), BF16),
        vmem((2, 256, 256), BF16),
        vmem((2, 8, 128), F32),
        vmem((8 * PITCH, 128), F32),
        vmem((64, 128), F32),
        vmem((16, 64, 128), BF16),
        vmem((16, 64, 128), BF16),
        vmem((64, 128), BF16),
        vmem((8, 64, 128), BF16),
        vmem((32, 64, 128), BF16),
        vmem((32, 64, 128), BF16),
        vmem((16, 64, 128), BF16),
        vmem((16, 64, 128), BF16),
        vmem((16, 64, 128), BF16),
        vmem((2, 16, 128), F32),
        vmem((2, 8, 128, 128), F32),
        vmem((256, 1024), F32),
        vmem((1024, 256), F32),
        vmem((256, 1024), BF16),
        vmem((256, 1024), BF16),
        vmem((4, 128, 256), F32),
        vmem((4, 128, 256), F32),
        vmem((4, 128, 256), F32),
        dma((4,)),
        dma((7,)),
        dma((8,)),
        dma((8,)),
        *[dma((16,)) for _ in range(12)],
        dma((4,)),
        dma((4,)),
        dma((2,)),
    ]
    return pl.pallas_call(
        kernel,
        out_shape=vmem(signal.shape, BF16),
        in_specs=[apart] * (4 + len(held)),
        out_specs=pl.BlockSpec(memory_space=pltpu.VMEM),
        scratch_shapes=scratch,
        compiler_params=pltpu.CompilerParams(collective_id=0, has_side_effects=True),
        name="hyena",
    )(signal, filter_taps, gate_values, skip_weight, *[jnp.asarray(t) for t in held])


def solution(mesh):
    shards = mesh.shape["ctx"]
    finer = Mesh(mesh.devices.reshape(shards, -1, 2), ("ctx", "x", "core"))
    chan = ("x", "core")
    placed = (P(chan, "ctx"), P(chan, "ctx"), P(chan, "ctx"), P(chan))
    return jax.shard_map(
        local, mesh=finer, in_specs=placed, out_specs=P(chan, "ctx"), check_vma=False
    )
```

```python
import functools

import jax
import jax.numpy as jnp
import ml_dtypes
import numpy as np
from jax import lax
from jax.experimental import pallas as pl
from jax.experimental.pallas import tpu as pltpu
from jax.sharding import Mesh
from jax.sharding import PartitionSpec as P

F32 = jnp.float32
BF16 = jnp.bfloat16
MESH = pl.DeviceIdType.MESH
PITCH = 136
HALF_ROOT = float(np.sqrt(0.5))


def two_parts(table):
    high = table.astype(ml_dtypes.bfloat16)
    low = (table - high.astype(np.float64)).astype(ml_dtypes.bfloat16)
    return np.stack([high, low])


@functools.cache
def tables():
    left, back, turn, step = [], [], [], []
    for core in range(2):
        shift = 0.125 + 0.5 * core
        kl = np.arange(128)[:, None] + shift
        angle = 2.0 * np.pi * np.mod(kl * np.arange(256)[None, :] / 128.0, 1.0)
        forward = np.concatenate([np.cos(angle), -np.sin(angle)], 0)
        left.append(two_parts(forward))
        inverse = np.roll(forward.T, -128 * core, 0)
        back.append(two_parts(inverse))
        angle = 2.0 * np.pi * np.mod(kl * np.arange(128)[None, :] / 131072.0, 1.0)
        turn.append(np.stack([np.cos(angle), -np.sin(angle)]))
        angle = np.broadcast_to(2.0 * np.pi * kl / 1024.0, (128, 128))
        step.append(np.stack([np.cos(angle), -np.sin(angle)]))
    index = np.arange(128)
    angle = 2.0 * np.pi * np.mod(index[:, None] * index[None, :] / 128.0, 1.0)
    cos, sin = np.cos(angle), np.sin(angle)
    right = two_parts(np.block([[cos, -sin], [sin, cos]]))
    undo = two_parts(np.block([[cos, sin], [-sin, cos]]) * 2.0**-18)
    angle = 2.0 * np.pi * np.arange(8)[:, None] * index[None, :] / 1024.0
    mid = np.stack([np.cos(angle), -np.sin(angle)])
    return (
        np.stack(left),
        np.stack(back),
        np.stack(turn).astype(np.float32),
        np.stack(step).astype(np.float32),
        right,
        undo,
        mid.astype(np.float32),
    )


def times(a, b):
    return (a[0] * b[0] - a[1] * b[1], a[0] * b[1] + a[1] * b[0])


def times_conj(a, b):
    return (a[0] * b[0] + a[1] * b[1], a[1] * b[0] - a[0] * b[1])


def plus(a, b):
    return (a[0] + b[0], a[1] + b[1])


def minus(a, b):
    return (a[0] - b[0], a[1] - b[1])


def quarter(a, sign):
    return (-a[1], a[0]) if sign > 0 else (a[1], -a[0])


def dft4(z, sign):
    even, odd = plus(z[0], z[2]), plus(z[1], z[3])
    d_even, d_odd = minus(z[0], z[2]), quarter(minus(z[1], z[3]), sign)
    return [plus(even, odd), plus(d_even, d_odd), minus(even, odd), minus(d_even, d_odd)]


def dft8(z, sign):
    low = [plus(z[j], z[j + 4]) for j in range(4)]
    high = [minus(z[j], z[j + 4]) for j in range(4)]
    h1 = plus(high[1], quarter(high[1], sign))
    h3 = minus(quarter(high[3], sign), high[3])
    high = [
        high[0],
        (h1[0] * HALF_ROOT, h1[1] * HALF_ROOT),
        quarter(high[2], sign),
        (h3[0] * HALF_ROOT, h3[1] * HALF_ROOT),
    ]
    even, odd = dft4(low, sign), dft4(high, sign)
    return [even[0], odd[0], even[1], odd[1], even[2], odd[2], even[3], odd[3]]


def split(value):
    high = value.astype(BF16)
    return high, (value - high.astype(F32)).astype(BF16)


def mm(a, b):
    return jnp.dot(a, b, preferred_element_type=F32)


def make_turns(turn, step, turns):
    def body(q, carry):
        rows = pl.ds(pl.multiple_of(q * 16, 16), 16)
        now = (turn[0, rows, :], turn[1, rows, :])
        by = (step[0, rows, :], step[1, rows, :])
        for a in range(8):
            turns[0, a, rows, :] = now[0]
            turns[1, a, rows, :] = now[1]
            if a < 7:
                now = times(now, by)
        return carry

    lax.fori_loop(0, 8, body, 0)


def first_stage(data, left, grid_f32):
    for c in range(4):
        tile = data[:, 16 * c : 16 * c + 16, :].astype(F32)
        block = jnp.concatenate(
            [tile[:, :8, :].reshape(256, 128), tile[:, 8:, :].reshape(256, 128)], axis=1
        ).astype(BF16)
        grid_f32[:, 256 * c : 256 * c + 256] = mm(left[0], block) + mm(left[1], block)


def second_stage(at, turns, mid, grid_f32):
    rows = slice(at, at + 16)
    z = []
    for a in range(8):
        cols = slice(128 * a, 128 * a + 128)
        value = (grid_f32[rows, cols], grid_f32[at + 128 : at + 144, cols])
        z.append(times(value, (turns[0, a, rows, :], turns[1, a, rows, :])))
    z = dft8(z, -1)
    for ka in range(1, 8):
        z[ka] = times(z[ka], (mid[0, ka : ka + 1, :], mid[1, ka : ka + 1, :]))
    return split(jnp.concatenate([jnp.concatenate(v, axis=1) for v in z], axis=0))


def transform_rows(m, right, turns, mid, grid_f32):
    parts = [second_stage(32 * m + 16 * o, turns, mid, grid_f32) for o in range(2)]
    high = jnp.concatenate([p[0] for p in parts], axis=0)
    low = jnp.concatenate([p[1] for p in parts], axis=0)
    return mm(high, right[0]) + mm(low, right[0]) + mm(high, right[1])


def spectrum_of(data, left, right, turns, mid, grid_f32, spectrum):
    first_stage(data, left, grid_f32)
    for m in range(4):
        spectrum[256 * m : 256 * m + 256, :] = transform_rows(m, right, turns, mid, grid_f32)


def middle(data, left, right, undo, turns, mid, grid_f32, spectrum, d_high, d_low):
    first_stage(data, left, grid_f32)
    for m in range(4):
        value = transform_rows(m, right, turns, mid, grid_f32)
        known = spectrum[256 * m : 256 * m + 256, :]
        re, im = times((value[:, :128], value[:, 128:]), (known[:, :128], known[:, 128:]))
        high, low = split(jnp.concatenate([re, im], axis=1))
        value = mm(high, undo[0]) + mm(low, undo[0]) + mm(high, undo[1])
        for o in range(2):
            at = 32 * m + 16 * o
            z = []
            for ka in range(8):
                rows = slice(128 * o + 16 * ka, 128 * o + 16 * ka + 16)
                z.append((value[rows, :128], value[rows, 128:]))
                if ka:
                    z[ka] = times_conj(z[ka], (mid[0, ka : ka + 1, :], mid[1, ka : ka + 1, :]))
            z = dft8(z, 1)
            for a in range(8):
                rows = slice(at, at + 16)
                back = times_conj(z[a], (turns[0, a, rows, :], turns[1, a, rows, :]))
                cols = slice(128 * a, 128 * a + 128)
                for part in range(2):
                    rows = slice(at + 128 * part, at + 128 * part + 16)
                    d_high[rows, cols], d_low[rows, cols] = split(back[part])


def inverse_columns(c, rows, back, d_high, d_low):
    cols = slice(256 * c, 256 * c + 256)
    high, low = d_high[:, cols], d_low[:, cols]
    return mm(back[0, rows, :], high) + mm(back[0, rows, :], low) + mm(back[1, rows, :], high)


def spread_out(rows_ref, work, send):
    for j in range(64):
        at = (j // 8) * PITCH + (j % 8) * 16
        work[at : at + 16, :] = rows_ref[:, 128 * j : 128 * j + 128].astype(F32)
    for r in range(16):
        for a in range(0, 8, 2):
            pair = [work[pl.ds((a + o) * 16 + r, 8, stride=PITCH), :] for o in range(2)]
            send[r, 8 * a : 8 * a + 16, :] = jnp.concatenate(pair, axis=0).astype(BF16)


def put_row(received, work, r):
    for a in range(0, 8, 2):
        pair = received[r, 8 * a : 8 * a + 16, :].astype(F32)
        for o in range(2):
            work[pl.ds((a + o) * 16 + r, 8, stride=PITCH), :] = pair[8 * o : 8 * o + 8, :]


def kernel(
    signal_in, taps_in, gate_in, skip_in, left_all, back_all, turn_all, step_all, right_all, undo_all, mid_all,
    out,
    signal, taps, gate, skip,
    left, back, turn, step, right, undo, mid,
    work, taps_work, send_x, send_g, send_t, ring_t, recv_x, recv_t, recv_g, send_o, recv_o, skips,
    turns, grid_f32, spectrum, d_high, d_low, y_mine, y_send, y_recv,
    input_sems, table_sems,
    sr, rr, sx, rx, st, rt, sg, rg, so, ro, fsx, frx, fst, frt, sy, ry, skip_sems,
):
    shard = lax.axis_index("ctx")
    core = lax.axis_index("core")
    half = lax.div(shard, 16)
    spot = lax.rem(shard, 16)
    first = 16 * core
    other = 16 - first
    mate = {"core": 1 - core}
    row = lax.div(shard, 8)
    col = lax.rem(shard, 8)

    def peer(i):
        return {"ctx": first + i, "core": half}

    def all_peers(body, unroll=1):
        def run(k, carry):
            body(lax.rem(spot + k, 16))
            return carry

        lax.fori_loop(0, 16, run, 0, unroll=unroll)

    barrier = pltpu.get_barrier_semaphore()

    def others(body):
        def run(i):
            @pl.when(first + i != shard)
            def _():
                body(i)

        all_peers(run)

    def ring(i):
        return {"ctx": row * 8 + i}

    def along_ring(body):
        def run(k, carry):
            body(lax.rem(col + k, 8))
            return carry

        lax.fori_loop(1, 8, run, 0)

    def hello(device):
        pl.semaphore_signal(barrier, inc=1, device_id=device, device_id_type=MESH)

    others(lambda i: hello(peer(i)))
    hello(mate)

    @pl.when(core != half)
    def _():
        along_ring(lambda i: hello(ring(i)))

    def fetch(pairs, sems):
        copies = [pltpu.make_async_copy(a, b, sems.at[i]) for i, (a, b) in enumerate(pairs)]
        for copy in copies:
            copy.start()
        return copies

    inputs = fetch(
        [(taps_in, taps), (signal_in, signal), (gate_in, gate), (skip_in, skip)], input_sems
    )
    copies = fetch(
        [
            (left_all.at[core], left),
            (turn_all.at[core], turn),
            (step_all.at[core], step),
            (right_all, right),
            (mid_all, mid),
            (undo_all, undo),
            (back_all.at[core], back),
        ],
        table_sems,
    )

    inputs[0].wait()
    for j in range(64):
        at = (j % 8) * 8 + j // 8
        taps_work[at : at + 1, :] = taps[:, 128 * j : 128 * j + 128].astype(F32)
    send_t[...] = taps_work[...].astype(BF16)
    inputs[1].wait()
    spread_out(signal, work, send_x)

    pl.semaphore_wait(barrier, jnp.where(core == half, 16, 24))

    def peer_copy(i, src, dst, send_sem, recv_sem):
        return pltpu.make_async_remote_copy(
            src_ref=src, dst_ref=dst, send_sem=send_sem.at[i], recv_sem=recv_sem,
            device_id=peer(i), device_id_type=MESH,
        )

    def ring_copy(i, slot):
        return pltpu.make_async_remote_copy(
            src_ref=send_t, dst_ref=ring_t.at[slot], send_sem=sr.at[i], recv_sem=rr.at[slot],
            device_id=ring(i), device_id_type=MESH,
        )

    def row_copy(block, side):
        i = side * 8 + col
        return pltpu.make_async_remote_copy(
            src_ref=ring_t.at[block], dst_ref=recv_t.at[row * 8 + block], send_sem=st.at[side * 8 + block],
            recv_sem=rt.at[lax.rem(row, 2) * 8 + block], device_id=peer(i), device_id_type=MESH,
        )

    def out_x(i):
        return peer_copy(i, send_x.at[i], recv_x.at[shard], sx, rx.at[spot])

    def out_g(i):
        return peer_copy(i, send_g.at[i], recv_g.at[spot], sg, rg.at[spot])

    def out_o(i):
        return peer_copy(i, send_o.at[i], recv_o.at[spot], so, ro.at[spot])

    def near(i):
        @pl.when(i != lax.rem(col + 4, 8))
        def _():
            ring_copy(i, col).start()

    along_ring(near)
    ring_t[col] = send_t[...]
    before = lax.rem(col + 5, 8)
    far = 8 + lax.rem(col + 4, 8)

    def in_order(body, unroll=1):
        def run(k, carry):
            i = lax.rem(far + k, 16)
            body(i)
            return carry

        lax.fori_loop(0, 16, run, 0, unroll=unroll)

    def from_far(body):
        def run(i):
            @pl.when(first + i != shard)
            def _():
                body(i)

        in_order(run)

    from_far(lambda i: out_x(i).start())

    @pl.when(core == half)
    def _():
        recv_x[shard] = send_x[spot]

    inputs[2].wait()
    spread_out(gate, work, send_g)
    inputs[3].wait()
    for r in range(16):
        skips[core, r : r + 1, :] = jnp.full((1, 128), skip[r], F32)
    skip_copy = pltpu.make_async_remote_copy(
        src_ref=skips.at[core], dst_ref=skips.at[core], send_sem=skip_sems.at[0],
        recv_sem=skip_sems.at[1], device_id=mate, device_id_type=MESH,
    )
    skip_copy.start()

    def incoming(i, slot, recv_sem):
        return peer_copy(i, send_t, slot, sx, recv_sem.at[i])

    def to_rows(block):
        for side in range(2):

            @pl.when(first + side * 8 + col != shard)
            def _():
                row_copy(block, side).start()

        @pl.when(core == half)
        def _():
            recv_t[row * 8 + block] = ring_t[block]

    to_rows(col)

    def ring_on(i):
        return pltpu.make_async_remote_copy(
            src_ref=ring_t.at[i], dst_ref=ring_t.at[i], send_sem=sr.at[col], recv_sem=rr.at[i],
            device_id=ring(lax.rem(col + 1, 8)), device_id_type=MESH,
        )

    def relay(i):
        ring_copy(i, i).wait_recv()

        @pl.when(i == before)
        def _():
            ring_on(i).start()

        to_rows(i)

    for k in (5, 1, 7, 2, 6, 3, 4):
        relay(lax.rem(col + k, 8))
    others(lambda i: out_g(i).start())

    @pl.when(core == half)
    def _():
        recv_g[spot] = send_g[spot]


    def to_mate(i, ref, slot, send_sem, recv_sem):
        return pltpu.make_async_remote_copy(
            src_ref=ref.at[slot], dst_ref=ref.at[slot], send_sem=send_sem.at[i],
            recv_sem=recv_sem.at[i], device_id=mate, device_id_type=MESH,
        )

    def hand_over(ref, recv_sem, fwd_send, fwd_recv, remote):
        def pass_on(i):
            @pl.when(remote(i))
            def _():
                incoming(i, ref.at[first + i], recv_sem).wait_recv()

            to_mate(i, ref, first + i, fwd_send, fwd_recv).start()

        all_peers(pass_on, 4)

    def take_over(ref, fwd_send, fwd_recv):
        for i in range(16):
            to_mate(i, ref, other + i, fwd_send, fwd_recv).wait_recv()

    for copy in copies:
        copy.wait()
    make_turns(turn, step, turns)

    hand_over(recv_x, rx, fsx, frx, lambda i: first + i != shard)
    hand_over(recv_t, rt, fst, frt, lambda i: lax.div(first + i, 8) != row)
    take_over(recv_x, fsx, frx)
    spectrum_of(recv_x, left, right, turns, mid, grid_f32, spectrum)
    take_over(recv_t, fst, frt)
    middle(recv_t, left, right, undo, turns, mid, grid_f32, spectrum, d_high, d_low)

    def y_copy(c):
        return pltpu.make_async_remote_copy(
            src_ref=y_send.at[c], dst_ref=y_recv.at[c], send_sem=sy.at[c], recv_sem=ry.at[c],
            device_id=mate, device_id_type=MESH,
        )

    for c in range(4):
        y_send[c] = inverse_columns(c, slice(128, 256), back, d_high, d_low)
        y_copy(c).start()
    for c in range(4):
        y_mine[c] = inverse_columns(c, slice(0, 128), back, d_high, d_low)
    skip_copy.wait()
    weight = skips[half, pl.ds(spot, 1), :]
    others(lambda i: incoming(i, recv_g.at[i], rg).wait_recv())
    for c in range(4):
        y_copy(c).wait_recv()

    def send_back(i):
        rows = pl.ds(pl.multiple_of(i * 8, 8), 8)
        for c in range(4):
            total = y_mine[c, rows, :] + y_recv[c, rows, :]
            total = jnp.concatenate([total[:, :128], total[:, 128:]], axis=0)
            cut = slice(16 * c, 16 * c + 16)
            direct = recv_x[first + i, cut, :].astype(F32)
            total = recv_g[i, cut, :].astype(F32) * (total + weight * direct)
            send_o[i, cut, :] = total.astype(BF16)

        @pl.when(first + i != shard)
        def _():
            out_o(i).start()

        @pl.when(first + i == shard)
        def _():
            recv_o[spot] = send_o[i]

    in_order(send_back, 4)

    def sent(i):
        out_x(i).wait_send()
        out_g(i).wait_send()
        out_o(i).wait_send()

    others(sent)

    def ring_sent(i):
        @pl.when(i != lax.rem(col + 4, 8))
        def _():
            ring_copy(i, col).wait_send()

    along_ring(ring_sent)
    ring_on(before).wait_send()

    def rows_sent(block, carry):
        for side in range(2):

            @pl.when(first + side * 8 + col != shard)
            def _():
                row_copy(block, side).wait_send()

        return carry

    lax.fori_loop(0, 8, rows_sent, 0)

    def passed(i, carry):
        to_mate(i, recv_t, first + i, fst, frt).wait_send()
        to_mate(i, recv_x, first + i, fsx, frx).wait_send()
        return carry

    lax.fori_loop(0, 16, passed, 0)
    for c in range(4):
        y_copy(c).wait_send()

    def place(i):
        @pl.when(first + i != shard)
        def _():
            incoming(i, recv_o.at[i], ro).wait_recv()

        put_row(recv_o, work, i)

    all_peers(place, 4)
    for j in range(64):
        at = (j // 8) * PITCH + (j % 8) * 16
        out[:, 128 * j : 128 * j + 128] = work[at : at + 16, :].astype(BF16)


def local(signal, filter_taps, gate_values, skip_weight):
    held = tables()
    vmem, dma = pltpu.VMEM, pltpu.SemaphoreType.DMA
    apart = pl.BlockSpec(memory_space=pl.ANY)
    scratch = [
        vmem((16, 8192), BF16),
        vmem((1, 8192), BF16),
        vmem((16, 8192), BF16),
        pltpu.SMEM((16,), F32),
        vmem((2, 256, 256), BF16),
        vmem((2, 256, 256), BF16),
        vmem((2, 128, 128), F32),
        vmem((2, 128, 128), F32),
        vmem((2, 256, 256), BF16),
        vmem((2, 256, 256), BF16),
        vmem((2, 8, 128), F32),
        vmem((8 * PITCH, 128), F32),
        vmem((64, 128), F32),
        vmem((16, 64, 128), BF16),
        vmem((16, 64, 128), BF16),
        vmem((64, 128), BF16),
        vmem((8, 64, 128), BF16),
        vmem((32, 64, 128), BF16),
        vmem((32, 64, 128), BF16),
        vmem((16, 64, 128), BF16),
        vmem((16, 64, 128), BF16),
        vmem((16, 64, 128), BF16),
        vmem((2, 16, 128), F32),
        vmem((2, 8, 128, 128), F32),
        vmem((256, 1024), F32),
        vmem((1024, 256), F32),
        vmem((256, 1024), BF16),
        vmem((256, 1024), BF16),
        vmem((4, 128, 256), F32),
        vmem((4, 128, 256), F32),
        vmem((4, 128, 256), F32),
        dma((4,)),
        dma((7,)),
        dma((8,)),
        dma((8,)),
        *[dma((16,)) for _ in range(12)],
        dma((4,)),
        dma((4,)),
        dma((2,)),
    ]
    return pl.pallas_call(
        kernel,
        out_shape=vmem(signal.shape, BF16),
        in_specs=[apart] * (4 + len(held)),
        out_specs=pl.BlockSpec(memory_space=pltpu.VMEM),
        scratch_shapes=scratch,
        compiler_params=pltpu.CompilerParams(collective_id=0, has_side_effects=True),
        name="hyena",
    )(signal, filter_taps, gate_values, skip_weight, *[jnp.asarray(t) for t in held])


def solution(mesh):
    shards = mesh.shape["ctx"]
    finer = Mesh(mesh.devices.reshape(shards, -1, 2), ("ctx", "x", "core"))
    chan = ("x", "core")
    placed = (P(chan, "ctx"), P(chan, "ctx"), P(chan, "ctx"), P(chan))
    return jax.shard_map(
        local, mesh=finer, in_specs=placed, out_specs=P(chan, "ctx"), check_vma=False
    )
```

```python
import functools

import jax
import jax.numpy as jnp
import ml_dtypes
import numpy as np
from jax import lax
from jax.experimental import pallas as pl
from jax.experimental.pallas import tpu as pltpu
from jax.sharding import Mesh
from jax.sharding import PartitionSpec as P

F32 = jnp.float32
BF16 = jnp.bfloat16
MESH = pl.DeviceIdType.MESH
PITCH = 136
HALF_ROOT = float(np.sqrt(0.5))


def two_parts(table):
    high = table.astype(ml_dtypes.bfloat16)
    low = (table - high.astype(np.float64)).astype(ml_dtypes.bfloat16)
    return np.stack([high, low])


@functools.cache
def tables():
    left, back, turn, step = [], [], [], []
    for core in range(2):
        shift = 0.125 + 0.5 * core
        kl = np.arange(128)[:, None] + shift
        angle = 2.0 * np.pi * np.mod(kl * np.arange(256)[None, :] / 128.0, 1.0)
        forward = np.concatenate([np.cos(angle), -np.sin(angle)], 0)
        left.append(two_parts(forward))
        inverse = np.roll(forward.T, -128 * core, 0)
        back.append(two_parts(inverse))
        angle = 2.0 * np.pi * np.mod(kl * np.arange(128)[None, :] / 131072.0, 1.0)
        turn.append(np.stack([np.cos(angle), -np.sin(angle)]))
        angle = np.broadcast_to(2.0 * np.pi * kl / 1024.0, (128, 128))
        step.append(np.stack([np.cos(angle), -np.sin(angle)]))
    index = np.arange(128)
    angle = 2.0 * np.pi * np.mod(index[:, None] * index[None, :] / 128.0, 1.0)
    cos, sin = np.cos(angle), np.sin(angle)
    right = two_parts(np.block([[cos, -sin], [sin, cos]]))
    undo = two_parts(np.block([[cos, sin], [-sin, cos]]) * 2.0**-18)
    angle = 2.0 * np.pi * np.arange(8)[:, None] * index[None, :] / 1024.0
    mid = np.stack([np.cos(angle), -np.sin(angle)])
    return (
        np.stack(left),
        np.stack(back),
        np.stack(turn).astype(np.float32),
        np.stack(step).astype(np.float32),
        right,
        undo,
        mid.astype(np.float32),
    )


def times(a, b):
    return (a[0] * b[0] - a[1] * b[1], a[0] * b[1] + a[1] * b[0])


def times_conj(a, b):
    return (a[0] * b[0] + a[1] * b[1], a[1] * b[0] - a[0] * b[1])


def plus(a, b):
    return (a[0] + b[0], a[1] + b[1])


def minus(a, b):
    return (a[0] - b[0], a[1] - b[1])


def quarter(a, sign):
    return (-a[1], a[0]) if sign > 0 else (a[1], -a[0])


def dft4(z, sign):
    even, odd = plus(z[0], z[2]), plus(z[1], z[3])
    d_even, d_odd = minus(z[0], z[2]), quarter(minus(z[1], z[3]), sign)
    return [plus(even, odd), plus(d_even, d_odd), minus(even, odd), minus(d_even, d_odd)]


def dft8(z, sign):
    low = [plus(z[j], z[j + 4]) for j in range(4)]
    high = [minus(z[j], z[j + 4]) for j in range(4)]
    h1 = plus(high[1], quarter(high[1], sign))
    h3 = minus(quarter(high[3], sign), high[3])
    high = [
        high[0],
        (h1[0] * HALF_ROOT, h1[1] * HALF_ROOT),
        quarter(high[2], sign),
        (h3[0] * HALF_ROOT, h3[1] * HALF_ROOT),
    ]
    even, odd = dft4(low, sign), dft4(high, sign)
    return [even[0], odd[0], even[1], odd[1], even[2], odd[2], even[3], odd[3]]


def split(value):
    high = value.astype(BF16)
    return high, (value - high.astype(F32)).astype(BF16)


def mm(a, b):
    return jnp.dot(a, b, preferred_element_type=F32)


def make_turns(turn, step, turns):
    def body(q, carry):
        rows = pl.ds(pl.multiple_of(q * 16, 16), 16)
        now = (turn[0, rows, :], turn[1, rows, :])
        by = (step[0, rows, :], step[1, rows, :])
        for a in range(8):
            turns[0, a, rows, :] = now[0]
            turns[1, a, rows, :] = now[1]
            if a < 7:
                now = times(now, by)
        return carry

    lax.fori_loop(0, 8, body, 0)


def first_stage(data, left, grid_f32):
    for c in range(4):
        tile = data[:, 16 * c : 16 * c + 16, :].astype(F32)
        block = jnp.concatenate(
            [tile[:, :8, :].reshape(256, 128), tile[:, 8:, :].reshape(256, 128)], axis=1
        ).astype(BF16)
        grid_f32[:, 256 * c : 256 * c + 256] = mm(left[0], block) + mm(left[1], block)


def second_stage(at, turns, mid, grid_f32):
    rows = slice(at, at + 16)
    z = []
    for a in range(8):
        cols = slice(128 * a, 128 * a + 128)
        value = (grid_f32[rows, cols], grid_f32[at + 128 : at + 144, cols])
        z.append(times(value, (turns[0, a, rows, :], turns[1, a, rows, :])))
    z = dft8(z, -1)
    for ka in range(1, 8):
        z[ka] = times(z[ka], (mid[0, ka : ka + 1, :], mid[1, ka : ka + 1, :]))
    return split(jnp.concatenate([jnp.concatenate(v, axis=1) for v in z], axis=0))


def transform_rows(m, right, turns, mid, grid_f32):
    parts = [second_stage(32 * m + 16 * o, turns, mid, grid_f32) for o in range(2)]
    high = jnp.concatenate([p[0] for p in parts], axis=0)
    low = jnp.concatenate([p[1] for p in parts], axis=0)
    return mm(high, right[0]) + mm(low, right[0]) + mm(high, right[1])


def spectrum_of(data, left, right, turns, mid, grid_f32, spectrum):
    first_stage(data, left, grid_f32)
    for m in range(4):
        spectrum[256 * m : 256 * m + 256, :] = transform_rows(m, right, turns, mid, grid_f32)


def middle(data, left, right, undo, turns, mid, grid_f32, spectrum, d_high, d_low):
    first_stage(data, left, grid_f32)
    for m in range(4):
        value = transform_rows(m, right, turns, mid, grid_f32)
        known = spectrum[256 * m : 256 * m + 256, :]
        re, im = times((value[:, :128], value[:, 128:]), (known[:, :128], known[:, 128:]))
        high, low = split(jnp.concatenate([re, im], axis=1))
        value = mm(high, undo[0]) + mm(low, undo[0]) + mm(high, undo[1])
        for o in range(2):
            at = 32 * m + 16 * o
            z = []
            for ka in range(8):
                rows = slice(128 * o + 16 * ka, 128 * o + 16 * ka + 16)
                z.append((value[rows, :128], value[rows, 128:]))
                if ka:
                    z[ka] = times_conj(z[ka], (mid[0, ka : ka + 1, :], mid[1, ka : ka + 1, :]))
            z = dft8(z, 1)
            for a in range(8):
                rows = slice(at, at + 16)
                back = times_conj(z[a], (turns[0, a, rows, :], turns[1, a, rows, :]))
                cols = slice(128 * a, 128 * a + 128)
                for part in range(2):
                    rows = slice(at + 128 * part, at + 128 * part + 16)
                    d_high[rows, cols], d_low[rows, cols] = split(back[part])


def inverse_columns(c, rows, back, d_high, d_low):
    cols = slice(256 * c, 256 * c + 256)
    high, low = d_high[:, cols], d_low[:, cols]
    return mm(back[0, rows, :], high) + mm(back[0, rows, :], low) + mm(back[1, rows, :], high)


def spread_out(rows_ref, work, send):
    for j in range(64):
        at = (j // 8) * PITCH + (j % 8) * 16
        work[at : at + 16, :] = rows_ref[:, 128 * j : 128 * j + 128].astype(F32)
    for r in range(16):
        for a in range(0, 8, 2):
            pair = [work[pl.ds((a + o) * 16 + r, 8, stride=PITCH), :] for o in range(2)]
            send[r, 8 * a : 8 * a + 16, :] = jnp.concatenate(pair, axis=0).astype(BF16)


def put_row(received, work, r):
    for a in range(0, 8, 2):
        pair = received[r, 8 * a : 8 * a + 16, :].astype(F32)
        for o in range(2):
            work[pl.ds((a + o) * 16 + r, 8, stride=PITCH), :] = pair[8 * o : 8 * o + 8, :]


def kernel(
    signal_in, taps_in, gate_in, skip_in, left_all, back_all, turn_all, step_all, right_all, undo_all, mid_all,
    out,
    signal, taps, gate, skip,
    left, back, turn, step, right, undo, mid,
    work, taps_work, send_x, send_g, send_t, ring_t, recv_x, recv_t, recv_g, send_o, recv_o, skips,
    turns, grid_f32, spectrum, d_high, d_low, y_mine, y_send, y_recv,
    input_sems, table_sems,
    sr, rr, sx, rx, st, rt, sg, rg, so, ro, fsx, frx, fst, frt, sy, ry, skip_sems,
):
    shard = lax.axis_index("ctx")
    core = lax.axis_index("core")
    half = lax.div(shard, 16)
    spot = lax.rem(shard, 16)
    first = 16 * core
    other = 16 - first
    mate = {"core": 1 - core}
    row = lax.div(shard, 8)
    col = lax.rem(shard, 8)

    def peer(i):
        return {"ctx": first + i, "core": half}

    def all_peers(body, unroll=4):
        def run(k, carry):
            body(lax.rem(spot + k, 16))
            return carry

        lax.fori_loop(0, 16, run, 0, unroll=unroll)

    barrier = pltpu.get_barrier_semaphore()

    def others(body):
        def run(i):
            @pl.when(first + i != shard)
            def _():
                body(i)

        all_peers(run)

    def ring(i):
        return {"ctx": row * 8 + i}

    def along_ring(body):
        def run(k, carry):
            body(lax.rem(col + k, 8))
            return carry

        lax.fori_loop(1, 8, run, 0, unroll=7)

    def hello(device):
        pl.semaphore_signal(barrier, inc=1, device_id=device, device_id_type=MESH)

    others(lambda i: hello(peer(i)))
    hello(mate)

    @pl.when(core != half)
    def _():
        along_ring(lambda i: hello(ring(i)))

    def fetch(pairs, sems):
        copies = [pltpu.make_async_copy(a, b, sems.at[i]) for i, (a, b) in enumerate(pairs)]
        for copy in copies:
            copy.start()
        return copies

    inputs = fetch(
        [(taps_in, taps), (signal_in, signal), (gate_in, gate), (skip_in, skip)], input_sems
    )
    copies = fetch(
        [
            (left_all.at[core], left),
            (turn_all.at[core], turn),
            (step_all.at[core], step),
            (right_all, right),
            (mid_all, mid),
            (undo_all, undo),
            (back_all.at[core], back),
        ],
        table_sems,
    )

    inputs[0].wait()
    for j in range(64):
        at = (j % 8) * 8 + j // 8
        taps_work[at : at + 1, :] = taps[:, 128 * j : 128 * j + 128].astype(F32)
    send_t[...] = taps_work[...].astype(BF16)
    inputs[1].wait()
    spread_out(signal, work, send_x)

    pl.semaphore_wait(barrier, jnp.where(core == half, 16, 24))

    def peer_copy(i, src, dst, send_sem, recv_sem):
        return pltpu.make_async_remote_copy(
            src_ref=src, dst_ref=dst, send_sem=send_sem.at[i], recv_sem=recv_sem,
            device_id=peer(i), device_id_type=MESH,
        )

    def ring_copy(i, slot):
        return pltpu.make_async_remote_copy(
            src_ref=send_t, dst_ref=ring_t.at[slot], send_sem=sr.at[i], recv_sem=rr.at[slot],
            device_id=ring(i), device_id_type=MESH,
        )

    def row_copy(block, side):
        i = side * 8 + col
        return pltpu.make_async_remote_copy(
            src_ref=ring_t.at[block], dst_ref=recv_t.at[row * 8 + block], send_sem=st.at[side * 8 + block],
            recv_sem=rt.at[lax.rem(row, 2) * 8 + block], device_id=peer(i), device_id_type=MESH,
        )

    def out_x(i):
        return peer_copy(i, send_x.at[i], recv_x.at[shard], sx, rx.at[spot])

    def out_g(i):
        return peer_copy(i, send_g.at[i], recv_g.at[spot], sg, rg.at[spot])

    def out_o(i):
        return peer_copy(i, send_o.at[i], recv_o.at[spot], so, ro.at[spot])

    def near(i):
        @pl.when(i != lax.rem(col + 4, 8))
        def _():
            ring_copy(i, col).start()

    along_ring(near)
    ring_t[col] = send_t[...]
    before = lax.rem(col + 5, 8)
    far = 8 + lax.rem(col + 4, 8)

    def in_order(body, unroll=4):
        def run(k, carry):
            i = lax.rem(far + k, 16)
            body(i)
            return carry

        lax.fori_loop(0, 16, run, 0, unroll=unroll)

    def from_far(body):
        def run(i):
            @pl.when(first + i != shard)
            def _():
                body(i)

        in_order(run)

    from_far(lambda i: out_x(i).start())

    @pl.when(core == half)
    def _():
        recv_x[shard] = send_x[spot]

    inputs[2].wait()
    spread_out(gate, work, send_g)
    inputs[3].wait()
    for r in range(16):
        skips[core, r : r + 1, :] = jnp.full((1, 128), skip[r], F32)
    skip_copy = pltpu.make_async_remote_copy(
        src_ref=skips.at[core], dst_ref=skips.at[core], send_sem=skip_sems.at[0],
        recv_sem=skip_sems.at[1], device_id=mate, device_id_type=MESH,
    )
    skip_copy.start()

    def incoming(i, slot, recv_sem):
        return peer_copy(i, send_t, slot, sx, recv_sem.at[i])

    def to_rows(block):
        for side in range(2):

            @pl.when(first + side * 8 + col != shard)
            def _():
                row_copy(block, side).start()

        @pl.when(core == half)
        def _():
            recv_t[row * 8 + block] = ring_t[block]

    to_rows(col)

    def ring_on(i):
        return pltpu.make_async_remote_copy(
            src_ref=ring_t.at[i], dst_ref=ring_t.at[i], send_sem=sr.at[col], recv_sem=rr.at[i],
            device_id=ring(lax.rem(col + 1, 8)), device_id_type=MESH,
        )

    def relay(i):
        ring_copy(i, i).wait_recv()

        @pl.when(i == before)
        def _():
            ring_on(i).start()

        to_rows(i)

    for k in (5, 1, 7, 2, 6, 3, 4):
        relay(lax.rem(col + k, 8))
    others(lambda i: out_g(i).start())

    @pl.when(core == half)
    def _():
        recv_g[spot] = send_g[spot]


    def to_mate(i, ref, slot, send_sem, recv_sem):
        return pltpu.make_async_remote_copy(
            src_ref=ref.at[slot], dst_ref=ref.at[slot], send_sem=send_sem.at[i],
            recv_sem=recv_sem.at[i], device_id=mate, device_id_type=MESH,
        )

    def hand_over(ref, recv_sem, fwd_send, fwd_recv, remote):
        def pass_on(i):
            @pl.when(remote(i))
            def _():
                incoming(i, ref.at[first + i], recv_sem).wait_recv()

            to_mate(i, ref, first + i, fwd_send, fwd_recv).start()

        all_peers(pass_on, 4)

    def take_over(ref, fwd_send, fwd_recv):
        for i in range(16):
            to_mate(i, ref, other + i, fwd_send, fwd_recv).wait_recv()

    for copy in copies:
        copy.wait()
    make_turns(turn, step, turns)

    hand_over(recv_x, rx, fsx, frx, lambda i: first + i != shard)
    hand_over(recv_t, rt, fst, frt, lambda i: lax.div(first + i, 8) != row)
    take_over(recv_x, fsx, frx)
    spectrum_of(recv_x, left, right, turns, mid, grid_f32, spectrum)
    take_over(recv_t, fst, frt)
    middle(recv_t, left, right, undo, turns, mid, grid_f32, spectrum, d_high, d_low)

    def y_copy(c):
        return pltpu.make_async_remote_copy(
            src_ref=y_send.at[c], dst_ref=y_recv.at[c], send_sem=sy.at[c], recv_sem=ry.at[c],
            device_id=mate, device_id_type=MESH,
        )

    for c in range(4):
        y_send[c] = inverse_columns(c, slice(128, 256), back, d_high, d_low)
        y_copy(c).start()
    for c in range(4):
        y_mine[c] = inverse_columns(c, slice(0, 128), back, d_high, d_low)
    skip_copy.wait()
    weight = skips[half, pl.ds(spot, 1), :]
    others(lambda i: incoming(i, recv_g.at[i], rg).wait_recv())
    for c in range(4):
        y_copy(c).wait_recv()

    def send_back(i):
        rows = pl.ds(pl.multiple_of(i * 8, 8), 8)
        for c in range(4):
            total = y_mine[c, rows, :] + y_recv[c, rows, :]
            total = jnp.concatenate([total[:, :128], total[:, 128:]], axis=0)
            cut = slice(16 * c, 16 * c + 16)
            direct = recv_x[first + i, cut, :].astype(F32)
            total = recv_g[i, cut, :].astype(F32) * (total + weight * direct)
            send_o[i, cut, :] = total.astype(BF16)

        @pl.when(first + i != shard)
        def _():
            out_o(i).start()

        @pl.when(first + i == shard)
        def _():
            recv_o[spot] = send_o[i]

    in_order(send_back, 4)

    def sent(i):
        out_x(i).wait_send()
        out_g(i).wait_send()
        out_o(i).wait_send()

    others(sent)

    def ring_sent(i):
        @pl.when(i != lax.rem(col + 4, 8))
        def _():
            ring_copy(i, col).wait_send()

    along_ring(ring_sent)
    ring_on(before).wait_send()

    def rows_sent(block, carry):
        for side in range(2):

            @pl.when(first + side * 8 + col != shard)
            def _():
                row_copy(block, side).wait_send()

        return carry

    lax.fori_loop(0, 8, rows_sent, 0)

    def passed(i, carry):
        to_mate(i, recv_t, first + i, fst, frt).wait_send()
        to_mate(i, recv_x, first + i, fsx, frx).wait_send()
        return carry

    lax.fori_loop(0, 16, passed, 0)
    for c in range(4):
        y_copy(c).wait_send()

    def place(i):
        @pl.when(first + i != shard)
        def _():
            incoming(i, recv_o.at[i], ro).wait_recv()

        put_row(recv_o, work, i)

    all_peers(place, 4)
    for j in range(64):
        at = (j // 8) * PITCH + (j % 8) * 16
        out[:, 128 * j : 128 * j + 128] = work[at : at + 16, :].astype(BF16)


def local(signal, filter_taps, gate_values, skip_weight):
    held = tables()
    vmem, dma = pltpu.VMEM, pltpu.SemaphoreType.DMA
    apart = pl.BlockSpec(memory_space=pl.ANY)
    scratch = [
        vmem((16, 8192), BF16),
        vmem((1, 8192), BF16),
        vmem((16, 8192), BF16),
        pltpu.SMEM((16,), F32),
        vmem((2, 256, 256), BF16),
        vmem((2, 256, 256), BF16),
        vmem((2, 128, 128), F32),
        vmem((2, 128, 128), F32),
        vmem((2, 256, 256), BF16),
        vmem((2, 256, 256), BF16),
        vmem((2, 8, 128), F32),
        vmem((8 * PITCH, 128), F32),
        vmem((64, 128), F32),
        vmem((16, 64, 128), BF16),
        vmem((16, 64, 128), BF16),
        vmem((64, 128), BF16),
        vmem((8, 64, 128), BF16),
        vmem((32, 64, 128), BF16),
        vmem((32, 64, 128), BF16),
        vmem((16, 64, 128), BF16),
        vmem((16, 64, 128), BF16),
        vmem((16, 64, 128), BF16),
        vmem((2, 16, 128), F32),
        vmem((2, 8, 128, 128), F32),
        vmem((256, 1024), F32),
        vmem((1024, 256), F32),
        vmem((256, 1024), BF16),
        vmem((256, 1024), BF16),
        vmem((4, 128, 256), F32),
        vmem((4, 128, 256), F32),
        vmem((4, 128, 256), F32),
        dma((4,)),
        dma((7,)),
        dma((8,)),
        dma((8,)),
        *[dma((16,)) for _ in range(12)],
        dma((4,)),
        dma((4,)),
        dma((2,)),
    ]
    return pl.pallas_call(
        kernel,
        out_shape=vmem(signal.shape, BF16),
        in_specs=[apart] * (4 + len(held)),
        out_specs=pl.BlockSpec(memory_space=pltpu.VMEM),
        scratch_shapes=scratch,
        compiler_params=pltpu.CompilerParams(collective_id=0, has_side_effects=True),
        name="hyena",
    )(signal, filter_taps, gate_values, skip_weight, *[jnp.asarray(t) for t in held])


def solution(mesh):
    shards = mesh.shape["ctx"]
    finer = Mesh(mesh.devices.reshape(shards, -1, 2), ("ctx", "x", "core"))
    chan = ("x", "core")
    placed = (P(chan, "ctx"), P(chan, "ctx"), P(chan, "ctx"), P(chan))
    return jax.shard_map(
        local, mesh=finer, in_specs=placed, out_specs=P(chan, "ctx"), check_vma=False
    )
```
